512 devices in a mesh: gx: 8 (over x, core), gy: 8 (over z_lo), gz: 8 (over z_hi, y).
Axes of the slice: x: 4, y: 4, z: 16 (z_hi: 2, z_lo: 8; z = z_hi * 8 + z_lo), core: 2. Of those that a mesh axis runs over, the one named last changes fastest.
Arguments:
- attn_out: bfloat16 [1408, 8192], P('gx', ('gz', 'gy')), may hold values from -6 to 6
- residual: bfloat16 [1408, 8192], P('gx', ('gy', 'gz')), may hold values from -60 to 60
- proj_weight: bfloat16 [8192, 8192], P(('gz', 'gx'), 'gy'), may hold values from -0.0625 to 0.0625
- norm_gain: float32 [8192], P(('gy', 'gz')), may hold values from 0.1 to 1.9
- gate_proj: bfloat16 [8192, 14336], P(('gy', 'gx'), 'gz'), may hold values from -0.0625 to 0.0625
- up_proj: bfloat16 [8192, 14336], P(('gy', 'gx'), 'gz'), may hold values from -0.0625 to 0.0625
- down_proj: bfloat16 [14336, 8192], P(('gz', 'gx'), 'gy'), may hold values from -0.046875 to 0.046875
Outputs:
- layer_out: bfloat16 [1408, 8192], P('gx', ('gy', 'gz'))
The draws below stay inside these ranges and needn't reach their ends.
All inputs are finite; a program needn't handle non-finite values.
Results may differ from the reference program's by a relative error of at most 0.0029.
Values may be sent and summed in bfloat16 or wider, within the bound.
A program may use at most 64 MiB of HBM per device.

```python
import jax
import jax.numpy as jnp
from jax import lax

D = 8192
FFW = 14336
TOKENS = 1408


def draw_residual(key, part):
    first, second = jax.random.split(key, 2)
    ramp = 1.0 + 2.0 * jnp.arange(D, dtype=jnp.float32)[None, :] / (D - 1)
    values = jnp.clip(jax.random.normal(first, (TOKENS, D), jnp.float32), -6.0, 6.0)
    scales = jnp.exp(jax.random.uniform(second, (TOKENS, 1), jnp.float32, jnp.log(0.3), jnp.log(3.0)))
    return (values * scales * ramp).astype(jnp.bfloat16)


def block_scale(rng, shape, shards, smallest, high):
    loudness, own = 1.0, jax.random.fold_in(rng, 6)
    for dim, parts in shards:
        steps = jnp.exp(jax.random.uniform(jax.random.fold_in(own, dim), (parts,), jnp.float32, smallest / len(shards), high / len(shards)))
        loudness = loudness * jnp.repeat(steps, shape[dim] // parts).reshape([-1 if axis == dim else 1 for axis in range(len(shape))])
    return loudness


def centred(rng, extent, scale, reach, cuts=(), held_as=jnp.bfloat16):
    factor_of = block_scale(rng, extent, cuts, -0.22, 0.18) if cuts else 1.0
    result = jax.random.normal(rng, extent, jnp.float32) * scale * factor_of
    return jnp.minimum(jnp.maximum(result, -reach), reach).astype(held_as)


def setup_inputs(seed: int = 0) -> dict:
    key_of = jax.random.split(jax.random.key(seed), 8)
    return {
        "attn_out": centred(key_of[0], (TOKENS, D), 1.0, 6.0, ((0, 8), (1, 64))),
        "residual": draw_residual(jax.random.fold_in(key_of[7], 71), 0),
        "proj_weight": centred(key_of[2], (D, D), D ** -0.5, 0.0625, ((0, 64), (1, 8))),
        "norm_gain": jnp.clip(1.0 + 0.18 * jax.random.normal(key_of[3], (D,), jnp.float32), 0.1, 1.9),
        "gate_proj": centred(key_of[4], (D, FFW), D ** -0.5, 0.0625, ((0, 64), (1, 8))),
        "up_proj": centred(key_of[5], (D, FFW), D ** -0.5, 0.0625, ((0, 64), (1, 8))),
        "down_proj": centred(key_of[6], (FFW, D), FFW ** -0.5, 0.046875, ((0, 64), (1, 8))),
    }


def reference(attn_out, residual, proj_weight, norm_gain, gate_proj, up_proj, down_proj):
    projected = jnp.dot(attn_out, proj_weight, preferred_element_type=jnp.float32)
    stream = residual.astype(jnp.float32) + projected
    inverse = lax.rsqrt(lax.optimization_barrier(jnp.mean(stream * stream, axis=1, keepdims=True)) + 1e-05)
    scaled = (stream * norm_gain.astype(jnp.float32)[None, :]).astype(jnp.bfloat16)
    gate_sum = inverse * jnp.dot(scaled, gate_proj, preferred_element_type=jnp.float32)
    up_sum = inverse * jnp.dot(scaled, up_proj, preferred_element_type=jnp.float32)
    hidden = (jax.nn.silu(gate_sum) * up_sum).astype(jnp.bfloat16)
    down_sum = jnp.dot(hidden, down_proj, preferred_element_type=jnp.float32)
    return (stream + down_sum).astype(jnp.bfloat16)
```

```python
import jax
import jax.numpy as jnp
from jax import lax
from jax.experimental import pallas as pl
from jax.experimental.pallas import tpu as pltpu
from jax.sharding import PartitionSpec as P

MESH = pl.DeviceIdType.MESH
D = 8192
ROWS, TILE = 176, 128
UNITS, UNIT = 7, 256
F32, BF16 = jnp.float32, jnp.bfloat16
X_STEPS = (2, 6, 4)


def rcopy(src, dst, send, recv, **where):
    return pltpu.make_async_remote_copy(
        src_ref=src, dst_ref=dst, send_sem=send, recv_sem=recv, device_id=where, device_id_type=MESH
    )


def signal(sem, **where):
    pl.semaphore_signal(sem, inc=1, device_id=where, device_id_type=MESH)


def dot(a, b):
    return jnp.dot(a, b, preferred_element_type=F32)


def kernel(
    attn_ref, res_ref, gain_ref, wp_hbm, wg_hbm, wu_hbm, wd_hbm, out_ref,
    attn_all, wp, wg, wu, wd, part8, y_send, y_recv, zh_send, zh_recv,
    gain_recv, stream, scaled, ssq_y, ssq_gy, inv, gu, acc_r, acc_l, hid, down,
    w_local, w_send, w_recv, w_fsend, w_frecv, a_send, a_recv, ys_send, ys_recv, ya_send, ya_recv,
    sy_send, sy_recv, sg_send, sg_recv, z_send, z_recv, r_send, r_recv, l_send, l_recv,
    hr_send, hl_send, h_recv,
):
    gx, gy, gz = lax.axis_index("gx"), lax.axis_index("gy"), lax.axis_index("gz")
    mate = gx + 1 - 2 * lax.rem(gx, 2)
    y, zh = lax.rem(gz, 4), gz // 4
    across = lax.rem(gz + 4, 8)
    up_chip, down_chip = lax.min(gy + 1, 7), lax.max(gy - 1, 0)

    weights = ((wp_hbm, wp), (wg_hbm, wg), (wu_hbm, wu), (wd_hbm, wd))

    def rows_of(w, who):
        depth = weights[w][0].shape[0]
        return weights[w][1].at[pl.ds(pl.multiple_of(who * depth, 16), depth)]

    def own_copy(w):
        return pltpu.make_async_copy(weights[w][0], rows_of(w, gx), w_local.at[w])

    for w in range(4):
        own_copy(w).start()

    barrier = pltpu.get_barrier_semaphore()
    for step in X_STEPS:
        signal(barrier, gx=lax.rem(gx + step, 8))
    signal(barrier, gx=mate)
    for d in range(1, 8):
        signal(barrier, gy=lax.rem(gy + d, 8))
    for d in range(1, 4):
        signal(barrier, gz=zh * 4 + lax.rem(y + d, 4))
    signal(barrier, gz=across)
    pl.semaphore_wait(barrier, 15)

    def attn_copy(d):
        return rcopy(attn_ref, attn_all.at[gy], a_send.at[d], a_recv.at[d], gy=lax.rem(gy + d, 8))

    def attn_arrival(d):
        who = lax.rem(gy + 8 - d, 8)
        return rcopy(attn_ref, attn_all.at[who], a_send.at[d], a_recv.at[d], gy=who)

    for d in range(1, 8):
        attn_copy(d).start()

    def w_copy(w, k):
        who = lax.rem(gx + X_STEPS[k], 8)
        return rcopy(weights[w][0], rows_of(w, gx), w_send.at[w, k], w_recv.at[w, k], gx=who)

    def w_arrival(w, k):
        who = lax.rem(gx + 8 - X_STEPS[k], 8)
        return rcopy(weights[w][0], rows_of(w, who), w_send.at[w, k], w_recv.at[w, k], gx=who)

    def w_mate(w, k):
        who = gx if k == 3 else lax.rem(gx + 8 - X_STEPS[k], 8)
        src = weights[w][0] if k == 3 else rows_of(w, who)
        return rcopy(src, rows_of(w, who), w_fsend.at[w, k], w_frecv.at[w, k], gx=mate)

    def w_mate_arrival(w, k):
        who = mate if k == 3 else lax.rem(mate + 8 - X_STEPS[k], 8)
        dst = rows_of(w, who)
        return rcopy(dst, dst, w_fsend.at[w, k], w_frecv.at[w, k], gx=mate)

    for w in range(4):
        for k in range(3):
            w_copy(w, k).start()
        w_mate(w, 3).start()

    def gain_copy():
        return rcopy(gain_ref, gain_recv, z_send.at[0], z_recv.at[0], gz=across)

    gain_copy().start()

    def forward(w):
        for k in range(3):
            w_arrival(w, k).wait_recv()
            w_mate(w, k).start()

    def weights_here(w):
        for k in range(4):
            w_mate_arrival(w, k).wait_recv()
        own_copy(w).wait()

    def y_copy(n, d):
        who = lax.rem(y + d, 4)
        return rcopy(
            y_send.at[n, who], y_recv.at[n, d - 1], ys_send.at[n, d - 1], ys_recv.at[n, d - 1],
            gz=zh * 4 + who,
        )

    def keep_tiles(n, m, total):
        for half in range(2):
            block = 2 * m + half
            tile = total[:, half * TILE : (half + 1) * TILE]
            part8[block] = tile
            y_send[n, block % 4, block // 4] = tile.astype(BF16)

    def y_sum(n, side):
        total = part8[side * 4 + y]
        for d in range(3):
            total += y_recv[n, d, side].astype(F32)
        return total

    attn_all[gy] = attn_ref[...]
    forward(0)
    for d in range(1, 8):
        attn_arrival(d).wait_recv()
    weights_here(0)
    for m in range(4):
        total = None
        for k in range(4):
            left = jnp.concatenate([attn_all[2 * k], attn_all[2 * k + 1]], axis=1)
            term = dot(left, wp[k * 256 : (k + 1) * 256, m * 256 : (m + 1) * 256])
            total = term if total is None else total + term
        keep_tiles(0, m, total)
    for d in range(1, 4):
        y_copy(0, d).start()
    for d in range(1, 4):
        y_copy(0, d).wait_recv()

    def zh_copy():
        return rcopy(zh_send.at[pl.ds(0, 2)], zh_recv.at[pl.ds(0, 2)], z_send.at[1], z_recv.at[1], gz=across)

    mine = res_ref[...].astype(F32) + y_sum(0, zh)
    theirs = y_sum(0, 1 - zh)
    zh_send[0] = mine.astype(BF16)
    zh_send[1] = theirs.astype(BF16)
    zh_copy().start()
    forward(1)
    gain_copy().wait_recv()
    zh_copy().wait_recv()
    mine += zh_recv[1].astype(F32)
    theirs += zh_recv[0].astype(F32)
    stream[...] = mine
    scaled[y, zh] = (mine * gain_ref[...]).astype(BF16)
    scaled[y, 1 - zh] = (theirs * gain_recv[...]).astype(BF16)

    def scaled_copy(d):
        who = zh * 4 + lax.rem(y + d, 4)
        return rcopy(scaled.at[y], scaled.at[y], ya_send.at[d], ya_recv.at[d], gz=who)

    def scaled_arrival(d):
        who = lax.rem(y + 4 - d, 4)
        return rcopy(scaled.at[who], scaled.at[who], ya_send.at[d], ya_recv.at[d], gz=zh * 4 + who)

    def ssq_copy(d):
        who = zh * 4 + lax.rem(y + d, 4)
        return rcopy(ssq_y.at[0], ssq_y.at[d], sy_send.at[d], sy_recv.at[d], gz=who)

    def ssq_gy_copy(d):
        who = lax.rem(gy + d, 8)
        return rcopy(ssq_gy.at[0], ssq_gy.at[d], sg_send.at[d], sg_recv.at[d], gy=who)

    for d in range(1, 4):
        scaled_copy(d).start()
    squares = jnp.sum(mine * mine + theirs * theirs, axis=1, keepdims=True)
    squares = jnp.concatenate(
        [jnp.broadcast_to(squares, (ROWS, TILE)), jnp.zeros((256 - ROWS, TILE), F32)], axis=0
    )
    ssq_y[0] = squares.T[:8]
    for d in range(1, 4):
        ssq_copy(d).start()
    for d in range(1, 4):
        scaled_arrival(d).wait_recv()
        ssq_copy(d).wait_recv()
    ssq_gy[0] = ssq_y[0] + ssq_y[1] + ssq_y[2] + ssq_y[3]
    for d in range(1, 8):
        ssq_gy_copy(d).start()

    forward(2)
    weights_here(1)
    weights_here(2)

    def products(unit):
        columns = pl.ds(pl.multiple_of(unit * UNIT, UNIT), UNIT)
        for part, w in enumerate((wg, wu)):
            total = None
            for k in range(4):
                a, b = 2 * k, 2 * k + 1
                left = jnp.concatenate([scaled[a % 4, a // 4], scaled[b % 4, b // 4]], axis=1)
                term = dot(left, w[k * 256 : (k + 1) * 256, columns])
                total = term if total is None else total + term
            gu[unit, part] = total

    def r_copy(unit, part):
        return rcopy(
            acc_r.at[unit, part], acc_r.at[unit, part], r_send.at[unit, part], r_recv.at[unit, part],
            gy=up_chip,
        )

    def l_copy(unit, part):
        return rcopy(
            acc_l.at[unit, part], acc_l.at[unit, part], l_send.at[unit, part], l_recv.at[unit, part],
            gy=down_chip,
        )

    def pass_on(unit, copy, acc, first):
        for part in range(2):

            @pl.when(first)
            def _():
                acc[unit, part] = gu[unit, part].astype(BF16)

            @pl.when(jnp.logical_not(first))
            def _():
                copy(unit, part).wait_recv()
                acc[unit, part] = (gu[unit, part] + acc[unit, part].astype(F32)).astype(BF16)

            copy(unit, part).start()

    def owner_of(unit):
        return unit + lax.min(lax.max(unit - 3, 0), 1)

    def line_step(t, carry):
        @pl.when(t < 4)
        def _():
            products(6 - t)

        @pl.when(t < 3)
        def _():
            products(t)

        right = 6 - t + gy

        @pl.when(jnp.logical_and(t >= gy, owner_of(right) > gy))
        def _():
            pass_on(right, r_copy, acc_r, gy == 0)

        left = t - 7 + gy

        @pl.when(jnp.logical_and(left >= 0, owner_of(left) < gy))
        def _():
            pass_on(left, l_copy, acc_l, gy == 7)

        return carry

    lax.fori_loop(0, 7, line_step, 0)

    for d in range(1, 8):
        ssq_gy_copy(d).wait_recv()
    total = ssq_gy[0]
    for d in range(1, 8):
        total += ssq_gy[d]
    total = lax.rsqrt(total[:1] / D + 1e-05)
    inv[...] = jnp.broadcast_to(total, (TILE, 256)).T

    owns = gy != 4
    own_unit = gy - lax.min(lax.max(gy - 4, 0), 1)

    @pl.when(owns)
    def _():
        for part in range(2):

            @pl.when(gy > 0)
            def _():
                r_copy(own_unit, part).wait_recv()
                gu[own_unit, part] += acc_r[own_unit, part].astype(F32)

            @pl.when(gy < 7)
            def _():
                l_copy(own_unit, part).wait_recv()
                gu[own_unit, part] += acc_l[own_unit, part].astype(F32)

        for half in range(2):
            columns = slice(half * TILE, (half + 1) * TILE)
            gate = inv[:ROWS] * gu[own_unit, 0, :, columns]
            up = inv[:ROWS] * gu[own_unit, 1, :, columns]
            hid[own_unit, half] = (gate / (1.0 + jnp.exp(-gate)) * up).astype(BF16)

    forward(3)
    weights_here(3)

    def hr_copy(unit, half):
        block = hid.at[unit, half]
        return rcopy(block, block, hr_send.at[unit, half], h_recv.at[unit, half], gy=up_chip)

    def hl_copy(unit, half):
        block = hid.at[unit, half]
        return rcopy(block, block, hl_send.at[unit, half], h_recv.at[unit, half], gy=down_chip)

    def add_down(unit):
        left = jnp.concatenate([hid[unit, 0], hid[unit, 1]], axis=1)
        rows = pl.ds(pl.multiple_of(unit * UNIT, UNIT), UNIT)
        for m in range(4):
            down[m] += dot(left, wd[rows, m * 256 : (m + 1) * 256])

    down[...] = jnp.zeros_like(down)

    @pl.when(owns)
    def _():
        for half in range(2):

            @pl.when(gy < 7)
            def _():
                hr_copy(own_unit, half).start()

            @pl.when(gy > 0)
            def _():
                hl_copy(own_unit, half).start()

        add_down(own_unit)

    def hidden_step(t, carry):
        from_left, from_right = gy - t, gy + t
        left_unit = from_left - lax.min(lax.max(from_left - 4, 0), 1)
        right_unit = from_right - lax.min(lax.max(from_right - 4, 0), 1)
        has_left = jnp.logical_and(from_left >= 0, from_left != 4)
        has_right = jnp.logical_and(from_right <= 7, from_right != 4)
        for has, unit, copy, more in (
            (has_left, left_unit, hr_copy, gy < 7), (has_right, right_unit, hl_copy, gy > 0)
        ):

            @pl.when(has)
            def _():
                for half in range(2):
                    copy(unit, half).wait_recv()

                    @pl.when(more)
                    def _():
                        copy(unit, half).start()

        for has, unit in ((has_left, left_unit), (has_right, right_unit)):

            @pl.when(has)
            def _():
                add_down(unit)

        return carry

    lax.fori_loop(1, 8, hidden_step, 0)

    for m in range(4):
        keep_tiles(1, m, down[m])
    for d in range(1, 4):
        y_copy(1, d).start()
    for d in range(1, 4):
        y_copy(1, d).wait_recv()

    def last_copy():
        return rcopy(zh_send.at[2], zh_recv.at[2], z_send.at[2], z_recv.at[2], gz=across)

    zh_send[2] = y_sum(1, 1 - zh).astype(BF16)
    last_copy().start()
    stream[...] += y_sum(1, zh)
    last_copy().wait_recv()
    out_ref[...] = (stream[...] + zh_recv[2].astype(F32)).astype(BF16)

    for d in range(1, 8):
        attn_copy(d).wait_send()
        ssq_gy_copy(d).wait_send()
    for w in range(4):
        for k in range(3):
            w_copy(w, k).wait_send()
            w_mate(w, k).wait_send()
        w_mate(w, 3).wait_send()
    for d in range(1, 4):
        y_copy(0, d).wait_send()
        y_copy(1, d).wait_send()
        scaled_copy(d).wait_send()
        ssq_copy(d).wait_send()
    gain_copy().wait_send()
    zh_copy().wait_send()
    last_copy().wait_send()

    def drain(unit, carry):
        owner = owner_of(unit)
        for part in range(2):

            @pl.when(owner > gy)
            def _():
                r_copy(unit, part).wait_send()

            @pl.when(owner < gy)
            def _():
                l_copy(unit, part).wait_send()

            @pl.when(jnp.logical_and(owner <= gy, gy < 7))
            def _():
                hr_copy(unit, part).wait_send()

            @pl.when(jnp.logical_and(owner >= gy, gy > 0))
            def _():
                hl_copy(unit, part).wait_send()

        return carry

    lax.fori_loop(0, UNITS, drain, 0)


def on_device(attn_out, residual, proj_weight, norm_gain, gate_proj, up_proj, down_proj):
    tile = (ROWS, TILE)
    in_vmem, in_hbm = pl.BlockSpec(memory_space=pltpu.VMEM), pl.BlockSpec(memory_space=pl.ANY)
    dma = pltpu.SemaphoreType.DMA
    return pl.pallas_call(
        kernel,
        out_shape=jax.ShapeDtypeStruct(tile, BF16),
        in_specs=[in_vmem] * 3 + [in_hbm] * 4,
        out_specs=in_vmem,
        scratch_shapes=[
            pltpu.VMEM((8, *tile), BF16),
            pltpu.VMEM((1024, 1024), BF16),
            pltpu.VMEM((1024, 1792), BF16),
            pltpu.VMEM((1024, 1792), BF16),
            pltpu.VMEM((1792, 1024), BF16),
            pltpu.VMEM((8, *tile), F32),
            pltpu.VMEM((2, 4, 2, *tile), BF16),
            pltpu.VMEM((2, 3, 2, *tile), BF16),
            pltpu.VMEM((3, *tile), BF16),
            pltpu.VMEM((3, *tile), BF16),
            pltpu.VMEM((1, TILE), F32),
            pltpu.VMEM(tile, F32),
            pltpu.VMEM((4, 2, *tile), BF16),
            pltpu.VMEM((4, 8, 256), F32),
            pltpu.VMEM((8, 8, 256), F32),
            pltpu.VMEM((256, TILE), F32),
            pltpu.VMEM((UNITS, 2, ROWS, UNIT), F32),
            pltpu.VMEM((UNITS, 2, ROWS, UNIT), BF16),
            pltpu.VMEM((UNITS, 2, ROWS, UNIT), BF16),
            pltpu.VMEM((UNITS, 2, *tile), BF16),
            pltpu.VMEM((4, ROWS, 256), F32),
            dma((4,)), dma((4, 3)), dma((4, 3)), dma((4, 4)), dma((4, 4)),
            dma((8,)), dma((8,)), dma((2, 3)), dma((2, 3)), dma((4,)), dma((4,)),
            dma((4,)), dma((4,)), dma((8,)), dma((8,)), dma((3,)), dma((3,)),
            dma((UNITS, 2)), dma((UNITS, 2)), dma((UNITS, 2)), dma((UNITS, 2)),
            dma((UNITS, 2)), dma((UNITS, 2)), dma((UNITS, 2)),
        ],
        compiler_params=pltpu.CompilerParams(
            collective_id=0, has_side_effects=True, vmem_limit_bytes=56 << 20
        ),
    )(attn_out, residual, norm_gain.reshape(1, TILE), proj_weight, gate_proj, up_proj, down_proj)


def solution(mesh):
    in_specs = (
        P("gx", ("gz", "gy")),
        P("gx", ("gy", "gz")),
        P(("gz", "gx"), "gy"),
        P(("gy", "gz")),
        P(("gy", "gx"), "gz"),
        P(("gy", "gx"), "gz"),
        P(("gz", "gx"), "gy"),
    )
    return jax.shard_map(
        on_device, mesh=mesh, in_specs=in_specs, out_specs=P("gx", ("gy", "gz")), check_vma=False
    )
```

```python
import jax
import jax.numpy as jnp
from jax import lax
from jax.experimental import pallas as pl
from jax.experimental.pallas import tpu as pltpu
from jax.sharding import PartitionSpec as P

MESH = pl.DeviceIdType.MESH
D = 8192
ROWS, TILE = 176, 128
UNITS, UNIT = 7, 256
F32, BF16 = jnp.float32, jnp.bfloat16
X_STEPS = (2, 6, 4)
PIECES = ((0, 96), (96, 80))


def rcopy(src, dst, send, recv, **where):
    return pltpu.make_async_remote_copy(
        src_ref=src, dst_ref=dst, send_sem=send, recv_sem=recv, device_id=where, device_id_type=MESH
    )


def signal(sem, **where):
    pl.semaphore_signal(sem, inc=1, device_id=where, device_id_type=MESH)


def dot(a, b):
    return jnp.dot(a, b, preferred_element_type=F32)


def kernel(
    attn_ref, res_ref, gain_ref, wp_hbm, wg_hbm, wu_hbm, wd_hbm, out_ref,
    attn_all, wp, wg, wu, wd, part8, y_send, y_recv, zh_send, zh_recv,
    gain_recv, stream, scaled, ssq_y, ssq_gy, inv, gu, acc_r, acc_l, hid, down,
    w_local, w_send, w_recv, w_psend, w_fsend, w_frecv, ar_send, al_send, a_recv, hello, ys_send, ys_recv, ya_send, ya_recv,
    sy_send, sy_recv, sg_send, sg_recv, z_send, z_recv, r_send, r_recv, l_send, l_recv,
    hr_send, hl_send, h_recv,
):
    gx, gy, gz = lax.axis_index("gx"), lax.axis_index("gy"), lax.axis_index("gz")
    mate = gx + 1 - 2 * lax.rem(gx, 2)
    y, zh = lax.rem(gz, 4), gz // 4
    across = lax.rem(gz + 4, 8)
    up_chip, down_chip = lax.min(gy + 1, 7), lax.max(gy - 1, 0)

    weights = ((wp_hbm, wp), (wg_hbm, wg), (wu_hbm, wu), (wd_hbm, wd))

    def rows_of(w, who):
        depth = weights[w][0].shape[0]
        return weights[w][1].at[pl.ds(pl.multiple_of(who * depth, 16), depth)]

    def own_copy(w):
        return pltpu.make_async_copy(weights[w][0], rows_of(w, gx), w_local.at[w])

    for w in range(4):
        own_copy(w).start()

    ahead = dict(gy=lax.rem(gy + 1, 8), gz=lax.select(gy == 7, across, gz))
    behind = dict(gy=lax.rem(gy + 7, 8), gz=lax.select(gy == 0, across, gz))
    barrier = pltpu.get_barrier_semaphore()
    for step in X_STEPS:
        signal(barrier, gx=lax.rem(gx + step, 8))
    signal(barrier, gx=mate)
    for d in range(1, 4):
        signal(barrier, gz=zh * 4 + lax.rem(y + d, 4))
    signal(barrier, **ahead)
    signal(barrier, **behind)
    pl.semaphore_wait(barrier, 9)
    signal(hello, **ahead)

    def attn_copy(block, piece, own, send, who):
        rows = pl.ds(*PIECES[piece])
        src = attn_ref.at[rows] if own else attn_all.at[block, rows]
        return rcopy(src, attn_all.at[block, rows], send.at[block, piece], a_recv.at[block, piece], gy=who)

    def ar_copy(block, piece, own=False):
        return attn_copy(block, piece, own, ar_send, up_chip)

    def al_copy(block, piece, own=False):
        return attn_copy(block, piece, own, al_send, down_chip)

    for piece in range(2):

        @pl.when(gy < 7)
        def _():
            ar_copy(gy, piece, True).start()

        @pl.when(gy > 0)
        def _():
            al_copy(gy, piece, True).start()

    def half_of(w, who, half):
        depth = weights[w][0].shape[0] // 2
        return weights[w][1].at[pl.ds(pl.multiple_of((2 * who + half) * depth, 16), depth)]

    def own_half(w, half):
        depth = weights[w][0].shape[0] // 2
        return weights[w][0].at[pl.ds(half * depth, depth)]

    def p_copy(k):
        who = lax.rem(gx + X_STEPS[k], 8)
        return rcopy(wp_hbm, rows_of(0, gx), w_psend.at[k, 0], w_psend.at[k, 1], gx=who)

    def p_arrival(k):
        who = lax.rem(gx + 8 - X_STEPS[k], 8)
        return rcopy(wp_hbm, rows_of(0, who), w_psend.at[k, 0], w_psend.at[k, 1], gx=who)

    def w_copy(w, k, half):
        who = lax.rem(gx + X_STEPS[k], 8)
        return rcopy(
            own_half(w, half), half_of(w, gx, half), w_send.at[w - 1, k, half], w_recv.at[w - 1, k, half], gx=who
        )

    def w_arrival(w, k, half):
        who = lax.rem(gx + 8 - X_STEPS[k], 8)
        dst = half_of(w, who, half)
        return rcopy(dst, dst, w_send.at[w - 1, k, half], w_recv.at[w - 1, k, half], gx=who)

    def w_onward(w, half):
        origin, who = lax.rem(gx + 8 - X_STEPS[half], 8), lax.rem(gx + X_STEPS[half], 8)
        block = half_of(w, origin, half)
        return rcopy(block, block, w_send.at[w - 1, 2, half], w_recv.at[w - 1, 2, half], gx=who)

    def w_onward_arrival(w, half):
        block = half_of(w, lax.rem(gx + 4, 8), half)
        who = lax.rem(gx + 8 - X_STEPS[half], 8)
        return rcopy(block, block, w_send.at[w - 1, 2, half], w_recv.at[w - 1, 2, half], gx=who)

    def w_mate(w, k):
        who = gx if k == 3 else lax.rem(gx + 8 - X_STEPS[k], 8)
        src = weights[w][0] if k == 3 else rows_of(w, who)
        return rcopy(src, rows_of(w, who), w_fsend.at[w, k], w_frecv.at[w, k], gx=mate)

    def w_mate_arrival(w, k):
        who = mate if k == 3 else lax.rem(mate + 8 - X_STEPS[k], 8)
        dst = rows_of(w, who)
        return rcopy(dst, dst, w_fsend.at[w, k], w_frecv.at[w, k], gx=mate)

    def send_own(w):
        for half in range(2):
            w_copy(w, 0, half).start()
            w_copy(w, 1, 1 - half).start()

    for k in range(3):
        p_copy(k).start()
    send_own(1)
    send_own(2)
    for w in range(4):
        w_mate(w, 3).start()

    def pass_weights(w):
        for half in range(2):
            w_arrival(w, half, half).wait_recv()
            w_onward(w, half).start()
        for k in range(2):
            w_arrival(w, k, 1 - k).wait_recv()
            w_mate(w, k).start()

    def last_weights(w):
        for half in range(2):
            w_onward_arrival(w, half).wait_recv()
        w_mate(w, 2).start()

    def weights_here(w):
        for k in range(4):
            w_mate_arrival(w, k).wait_recv()
        own_copy(w).wait()

    def attn_step(t, carry):
        for piece in range(2):
            for has, block, copy, more in (
                (gy >= t, gy - t, ar_copy, gy < 7), (gy + t <= 7, gy + t, al_copy, gy > 0)
            ):

                @pl.when(has)
                def _():
                    copy(block, piece).wait_recv()

                    @pl.when(more)
                    def _():
                        copy(block, piece).start()

        pl.semaphore_wait(hello, 1)
        signal(hello, **ahead)

        @pl.when(t == 5)
        def _():
            for k in range(2):
                p_arrival(k).wait_recv()
                w_mate(0, k).start()

        return carry

    attn_all[gy] = attn_ref[...]
    lax.fori_loop(1, 8, attn_step, 0)
    p_arrival(2).wait_recv()
    w_mate(0, 2).start()
    pl.semaphore_wait(hello, 1)

    def gain_copy():
        return rcopy(gain_ref, gain_recv, z_send.at[0], z_recv.at[0], gz=across)

    gain_copy().start()

    def y_copy(n, d):
        who = lax.rem(y + d, 4)
        return rcopy(
            y_send.at[n, who], y_recv.at[n, d - 1], ys_send.at[n, d - 1], ys_recv.at[n, d - 1],
            gz=zh * 4 + who,
        )

    def keep_tiles(n, m, total):
        for half in range(2):
            block = 2 * m + half
            tile = total[:, half * TILE : (half + 1) * TILE]
            part8[block] = tile
            y_send[n, block % 4, block // 4] = tile.astype(BF16)

    def y_sum(n, side):
        total = part8[side * 4 + y]
        for d in range(3):
            total += y_recv[n, d, side].astype(F32)
        return total

    weights_here(0)
    for m in range(4):
        total = None
        for k in range(4):
            left = jnp.concatenate([attn_all[2 * k], attn_all[2 * k + 1]], axis=1)
            term = dot(left, wp[k * 256 : (k + 1) * 256, m * 256 : (m + 1) * 256])
            total = term if total is None else total + term
        keep_tiles(0, m, total)
    for d in range(1, 4):
        y_copy(0, d).start()
    pass_weights(1)
    for d in range(1, 4):
        y_copy(0, d).wait_recv()

    def zh_copy():
        return rcopy(zh_send.at[pl.ds(0, 2)], zh_recv.at[pl.ds(0, 2)], z_send.at[1], z_recv.at[1], gz=across)

    mine = res_ref[...].astype(F32) + y_sum(0, zh)
    theirs = y_sum(0, 1 - zh)
    zh_send[0] = mine.astype(BF16)
    zh_send[1] = theirs.astype(BF16)
    zh_copy().start()
    pass_weights(2)
    send_own(3)
    last_weights(1)
    gain_copy().wait_recv()
    zh_copy().wait_recv()
    mine += zh_recv[1].astype(F32)
    theirs += zh_recv[0].astype(F32)
    stream[...] = mine
    scaled[y, zh] = (mine * gain_ref[...]).astype(BF16)
    scaled[y, 1 - zh] = (theirs * gain_recv[...]).astype(BF16)

    def scaled_copy(d):
        who = zh * 4 + lax.rem(y + d, 4)
        return rcopy(scaled.at[y], scaled.at[y], ya_send.at[d], ya_recv.at[d], gz=who)

    def scaled_arrival(d):
        who = lax.rem(y + 4 - d, 4)
        return rcopy(scaled.at[who], scaled.at[who], ya_send.at[d], ya_recv.at[d], gz=zh * 4 + who)

    def ssq_copy(d):
        who = zh * 4 + lax.rem(y + d, 4)
        return rcopy(ssq_y.at[0], ssq_y.at[d], sy_send.at[d], sy_recv.at[d], gz=who)

    def ssq_gy_copy(d):
        who = lax.rem(gy + d, 8)
        return rcopy(ssq_gy.at[0], ssq_gy.at[d], sg_send.at[d], sg_recv.at[d], gy=who)

    for d in range(1, 4):
        scaled_copy(d).start()
    squares = jnp.sum(mine * mine + theirs * theirs, axis=1, keepdims=True)
    squares = jnp.concatenate(
        [jnp.broadcast_to(squares, (ROWS, TILE)), jnp.zeros((256 - ROWS, TILE), F32)], axis=0
    )
    ssq_y[0] = squares.T[:8]
    for d in range(1, 4):
        ssq_copy(d).start()
    last_weights(2)
    for d in range(1, 4):
        scaled_arrival(d).wait_recv()
        ssq_copy(d).wait_recv()
    ssq_gy[0] = (ssq_y[0] + ssq_y[1] + ssq_y[2] + ssq_y[3])[:1]
    for d in range(1, 8):
        ssq_gy_copy(d).start()

    weights_here(1)
    weights_here(2)

    def products(unit):
        columns = pl.ds(pl.multiple_of(unit * UNIT, UNIT), UNIT)
        for part, w in enumerate((wg, wu)):
            total = None
            for k in range(4):
                a, b = 2 * k, 2 * k + 1
                left = jnp.concatenate([scaled[a % 4, a // 4], scaled[b % 4, b // 4]], axis=1)
                term = dot(left, w[k * 256 : (k + 1) * 256, columns])
                total = term if total is None else total + term
            for half in range(2):
                gu[unit, 2 * part + half] = total[:, half * TILE : (half + 1) * TILE]

    def r_copy(unit, part):
        return rcopy(
            acc_r.at[unit, part], acc_r.at[unit, part], r_send.at[unit, part], r_recv.at[unit, part],
            gy=up_chip,
        )

    def l_copy(unit, part):
        return rcopy(
            acc_l.at[unit, part], acc_l.at[unit, part], l_send.at[unit, part], l_recv.at[unit, part],
            gy=down_chip,
        )

    def pass_on(tile, unit, copy, acc, first):
        @pl.when(first)
        def _():
            acc[unit, tile] = gu[unit, tile].astype(BF16)

        @pl.when(jnp.logical_not(first))
        def _():
            copy(unit, tile).wait_recv()
            acc[unit, tile] = (gu[unit, tile] + acc[unit, tile].astype(F32)).astype(BF16)

        copy(unit, tile).start()

    def owner_of(unit):
        return unit + lax.min(lax.max(unit - 3, 0), 1)

    def line_step(t, carry):
        @pl.when(t < 4)
        def _():
            products(lax.select(gy < 4, 6 - t, t))

        right, left = 6 - t + gy, t - 7 + gy
        for tile in range(4):

            @pl.when(jnp.logical_and(t >= gy, owner_of(right) > gy))
            def _():
                pass_on(tile, right, r_copy, acc_r, gy == 0)

            @pl.when(jnp.logical_and(left >= 0, owner_of(left) < gy))
            def _():
                pass_on(tile, left, l_copy, acc_l, gy == 7)

        @pl.when(t < 3)
        def _():
            products(lax.select(gy < 4, t, 6 - t))

        @pl.when(t == 2)
        def _():
            pass_weights(3)

        @pl.when(t == 5)
        def _():
            last_weights(3)

        return carry

    lax.fori_loop(0, 7, line_step, 0)

    for d in range(1, 8):
        ssq_gy_copy(d).wait_recv()
    total = ssq_gy[0]
    for d in range(1, 8):
        total += ssq_gy[d]
    total = lax.rsqrt(total / D + 1e-05)
    inv[...] = jnp.broadcast_to(total, (TILE, 256)).T

    owns = gy != 4
    own_unit = gy - lax.min(lax.max(gy - 4, 0), 1)

    @pl.when(owns)
    def _():
        for tile in range(4):

            @pl.when(gy > 0)
            def _():
                r_copy(own_unit, tile).wait_recv()
                gu[own_unit, tile] += acc_r[own_unit, tile].astype(F32)

            @pl.when(gy < 7)
            def _():
                l_copy(own_unit, tile).wait_recv()
                gu[own_unit, tile] += acc_l[own_unit, tile].astype(F32)

        for half in range(2):
            gate = inv[:ROWS] * gu[own_unit, half]
            up = inv[:ROWS] * gu[own_unit, 2 + half]
            hid[own_unit, half] = (gate / (1.0 + jnp.exp(-gate)) * up).astype(BF16)

    weights_here(3)

    def hidden_copy(unit, k, send, who):
        half, piece = k // 2, k % 2
        block = hid.at[unit, half, pl.ds(*PIECES[piece])]
        return rcopy(block, block, send.at[unit, k], h_recv.at[unit, k], gy=who)

    def hr_copy(unit, k):
        return hidden_copy(unit, k, hr_send, up_chip)

    def hl_copy(unit, k):
        return hidden_copy(unit, k, hl_send, down_chip)

    def add_down(unit):
        left = jnp.concatenate([hid[unit, 0], hid[unit, 1]], axis=1)
        rows = pl.ds(pl.multiple_of(unit * UNIT, UNIT), UNIT)
        for m in range(4):
            down[m] += dot(left, wd[rows, m * 256 : (m + 1) * 256])

    down[...] = jnp.zeros_like(down)

    @pl.when(owns)
    def _():
        for k in range(4):

            @pl.when(gy < 7)
            def _():
                hr_copy(own_unit, k).start()

            @pl.when(gy > 0)
            def _():
                hl_copy(own_unit, k).start()

        add_down(own_unit)

    def hidden_step(t, carry):
        from_left, from_right = gy - t, gy + t
        left_unit = from_left - lax.min(lax.max(from_left - 4, 0), 1)
        right_unit = from_right - lax.min(lax.max(from_right - 4, 0), 1)
        has_left = jnp.logical_and(from_left >= 0, from_left != 4)
        has_right = jnp.logical_and(from_right <= 7, from_right != 4)
        for k in range(4):
            for has, unit, copy, more in (
                (has_left, left_unit, hr_copy, gy < 7), (has_right, right_unit, hl_copy, gy > 0)
            ):

                @pl.when(has)
                def _():
                    copy(unit, k).wait_recv()

                    @pl.when(more)
                    def _():
                        copy(unit, k).start()

        for has, unit in ((has_left, left_unit), (has_right, right_unit)):

            @pl.when(has)
            def _():
                add_down(unit)

        return carry

    lax.fori_loop(1, 8, hidden_step, 0)

    for m in range(4):
        keep_tiles(1, m, down[m])
    for d in range(1, 4):
        y_copy(1, d).start()
    for d in range(1, 4):
        y_copy(1, d).wait_recv()

    def last_copy():
        return rcopy(zh_send.at[2], zh_recv.at[2], z_send.at[2], z_recv.at[2], gz=across)

    zh_send[2] = y_sum(1, 1 - zh).astype(BF16)
    last_copy().start()
    stream[...] += y_sum(1, zh)
    last_copy().wait_recv()
    out_ref[...] = (stream[...] + zh_recv[2].astype(F32)).astype(BF16)

    for d in range(1, 8):
        ssq_gy_copy(d).wait_send()
    for k in range(3):
        p_copy(k).wait_send()
    for w in range(4):
        for k in range(4):
            w_mate(w, k).wait_send()
    for w in range(1, 4):
        for half in range(2):
            w_copy(w, 0, half).wait_send()
            w_copy(w, 1, half).wait_send()
            w_onward(w, half).wait_send()
    for d in range(1, 4):
        y_copy(0, d).wait_send()
        y_copy(1, d).wait_send()
        scaled_copy(d).wait_send()
        ssq_copy(d).wait_send()
    gain_copy().wait_send()
    zh_copy().wait_send()
    last_copy().wait_send()

    def drain(unit, carry):
        owner = owner_of(unit)
        for k in range(4):

            @pl.when(owner > gy)
            def _():
                r_copy(unit, k).wait_send()

            @pl.when(owner < gy)
            def _():
                l_copy(unit, k).wait_send()

            @pl.when(jnp.logical_and(owner <= gy, gy < 7))
            def _():
                hr_copy(unit, k).wait_send()

            @pl.when(jnp.logical_and(owner >= gy, gy > 0))
            def _():
                hl_copy(unit, k).wait_send()

        return carry

    lax.fori_loop(0, UNITS, drain, 0)

    def drain_attn(block, carry):
        for piece in range(2):

            @pl.when(jnp.logical_and(block <= gy, gy < 7))
            def _():
                ar_copy(block, piece).wait_send()

            @pl.when(jnp.logical_and(block >= gy, gy > 0))
            def _():
                al_copy(block, piece).wait_send()

        return carry

    lax.fori_loop(0, 8, drain_attn, 0)


def on_device(attn_out, residual, proj_weight, norm_gain, gate_proj, up_proj, down_proj):
    tile = (ROWS, TILE)
    in_vmem, in_hbm = pl.BlockSpec(memory_space=pltpu.VMEM), pl.BlockSpec(memory_space=pl.ANY)
    dma = pltpu.SemaphoreType.DMA
    return pl.pallas_call(
        kernel,
        out_shape=jax.ShapeDtypeStruct(tile, BF16),
        in_specs=[in_vmem] * 3 + [in_hbm] * 4,
        out_specs=in_vmem,
        scratch_shapes=[
            pltpu.VMEM((8, *tile), BF16),
            pltpu.VMEM((1024, 1024), BF16),
            pltpu.VMEM((1024, 1792), BF16),
            pltpu.VMEM((1024, 1792), BF16),
            pltpu.VMEM((1792, 1024), BF16),
            pltpu.VMEM((8, *tile), F32),
            pltpu.VMEM((2, 4, 2, *tile), BF16),
            pltpu.VMEM((2, 3, 2, *tile), BF16),
            pltpu.VMEM((3, *tile), BF16),
            pltpu.VMEM((3, *tile), BF16),
            pltpu.VMEM((1, TILE), F32),
            pltpu.VMEM(tile, F32),
            pltpu.VMEM((4, 2, *tile), BF16),
            pltpu.VMEM((4, 8, 256), F32),
            pltpu.VMEM((8, 1, 256), F32),
            pltpu.VMEM((256, TILE), F32),
            pltpu.VMEM((UNITS, 4, *tile), F32),
            pltpu.VMEM((UNITS, 4, *tile), BF16),
            pltpu.VMEM((UNITS, 4, *tile), BF16),
            pltpu.VMEM((UNITS, 2, *tile), BF16),
            pltpu.VMEM((4, ROWS, 256), F32),
            dma((4,)), dma((3, 3, 2)), dma((3, 3, 2)), dma((3, 2)), dma((4, 4)), dma((4, 4)),
            dma((8, 2)), dma((8, 2)), dma((8, 2)), pltpu.SemaphoreType.REGULAR,
            dma((2, 3)), dma((2, 3)), dma((4,)), dma((4,)),
            dma((4,)), dma((4,)), dma((8,)), dma((8,)), dma((3,)), dma((3,)),
            dma((UNITS, 4)), dma((UNITS, 4)), dma((UNITS, 4)), dma((UNITS, 4)),
            dma((UNITS, 4)), dma((UNITS, 4)), dma((UNITS, 4)),
        ],
        compiler_params=pltpu.CompilerParams(
            collective_id=0, has_side_effects=True, vmem_limit_bytes=56 << 20
        ),
    )(attn_out, residual, norm_gain.reshape(1, TILE), proj_weight, gate_proj, up_proj, down_proj)


def solution(mesh):
    in_specs = (
        P("gx", ("gz", "gy")),
        P("gx", ("gy", "gz")),
        P(("gz", "gx"), "gy"),
        P(("gy", "gz")),
        P(("gy", "gx"), "gz"),
        P(("gy", "gx"), "gz"),
        P(("gz", "gx"), "gy"),
    )
    return jax.shard_map(
        on_device, mesh=mesh, in_specs=in_specs, out_specs=P("gx", ("gy", "gz")), check_vma=False
    )
```

```python
import jax
import jax.numpy as jnp
from jax import lax
from jax.experimental import pallas as pl
from jax.experimental.pallas import tpu as pltpu
from jax.sharding import PartitionSpec as P

MESH = pl.DeviceIdType.MESH
D = 8192
ROWS, TILE = 176, 128
UNITS, UNIT = 7, 256
F32, BF16 = jnp.float32, jnp.bfloat16
X_STEPS = (2, 6, 4)
PIECES = ((0, 96), (96, 80))


def rcopy(src, dst, send, recv, **where):
    return pltpu.make_async_remote_copy(
        src_ref=src, dst_ref=dst, send_sem=send, recv_sem=recv, device_id=where, device_id_type=MESH
    )


def signal(sem, **where):
    pl.semaphore_signal(sem, inc=1, device_id=where, device_id_type=MESH)


def dot(a, b):
    return jnp.dot(a, b, preferred_element_type=F32)


def kernel(
    attn_ref, res_ref, gain_ref, wp_hbm, wg_hbm, wu_hbm, wd_hbm, out_ref,
    attn_all, wp, wg, wu, wd, part8, y_send, y_recv, zh_send, zh_recv,
    gain_recv, stream, scaled, ssq_y, ssq_gy, inv, gu, acc_r, acc_l, hid, down,
    w_local, w_send, w_recv, w_fsend, w_frecv, a_send, a_recv, hello, ys_send, ys_recv, ya_send, ya_recv,
    sy_send, sy_recv, sg_send, sg_recv, z_send, z_recv, r_send, r_recv, l_send, l_recv,
    h_send, h_recv,
):
    gx, gy, gz = lax.axis_index("gx"), lax.axis_index("gy"), lax.axis_index("gz")
    mate = gx + 1 - 2 * lax.rem(gx, 2)
    y, zh = lax.rem(gz, 4), gz // 4
    across = lax.rem(gz + 4, 8)
    up_chip, down_chip = lax.min(gy + 1, 7), lax.max(gy - 1, 0)

    weights = ((wp_hbm, wp), (wg_hbm, wg), (wu_hbm, wu), (wd_hbm, wd))

    def rows_of(w, who):
        depth = weights[w][0].shape[0]
        return weights[w][1].at[pl.ds(pl.multiple_of(who * depth, 16), depth)]

    def own_copy(w):
        return pltpu.make_async_copy(weights[w][0], rows_of(w, gx), w_local.at[w])

    for w in range(4):
        own_copy(w).start()

    far_gy, quad, place = lax.rem(gy + 4, 8), gy // 4 * 4, lax.rem(gy, 4)

    def in_quad(d):
        return quad + lax.rem(place + d, 4)

    barrier = pltpu.get_barrier_semaphore()
    for step in X_STEPS:
        signal(barrier, gx=lax.rem(gx + step, 8))
    signal(barrier, gx=mate)
    for d in range(1, 4):
        signal(barrier, gz=zh * 4 + lax.rem(y + d, 4))
        signal(barrier, gy=in_quad(d))
    signal(barrier, gy=far_gy)
    signal(barrier, gy=far_gy, gz=across)
    pl.semaphore_wait(barrier, 12)
    signal(hello, gy=far_gy, gz=across)

    def attn_far():
        return rcopy(attn_ref, attn_all.at[gy], a_send.at[0], a_recv.at[0], gy=far_gy)

    def attn_far_arrival():
        return rcopy(attn_ref, attn_all.at[far_gy], a_send.at[0], a_recv.at[0], gy=far_gy)

    def attn_near(d):
        return rcopy(attn_ref, attn_all.at[gy], a_send.at[d], a_recv.at[d], gy=in_quad(d))

    def attn_onward(d):
        block = attn_all.at[far_gy]
        return rcopy(block, block, a_send.at[3 + d], a_recv.at[3 + d], gy=in_quad(d))

    def attn_arrival(d, onward):
        who = in_quad(4 - d)
        block = attn_all.at[lax.rem(who + 4, 8) if onward else who]
        k = d + 3 if onward else d
        return rcopy(block, block, a_send.at[k], a_recv.at[k], gy=who)

    attn_far().start()
    for d in range(1, 4):
        attn_near(d).start()

    def half_of(w, who, half):
        depth = weights[w][0].shape[0] // 2
        return weights[w][1].at[pl.ds(pl.multiple_of((2 * who + half) * depth, 16), depth)]

    def own_half(w, half):
        depth = weights[w][0].shape[0] // 2
        return weights[w][0].at[pl.ds(half * depth, depth)]

    def w_copy(w, k, half):
        who = lax.rem(gx + X_STEPS[k], 8)
        return rcopy(
            own_half(w, half), half_of(w, gx, half), w_send.at[w, k, half], w_recv.at[w, k, half], gx=who
        )

    def w_arrival(w, k, half):
        who = lax.rem(gx + 8 - X_STEPS[k], 8)
        dst = half_of(w, who, half)
        return rcopy(dst, dst, w_send.at[w, k, half], w_recv.at[w, k, half], gx=who)

    def w_onward(w, half):
        origin, who = lax.rem(gx + 8 - X_STEPS[half], 8), lax.rem(gx + X_STEPS[half], 8)
        block = half_of(w, origin, half)
        return rcopy(block, block, w_send.at[w, 2, half], w_recv.at[w, 2, half], gx=who)

    def w_onward_arrival(w, half):
        block = half_of(w, lax.rem(gx + 4, 8), half)
        who = lax.rem(gx + 8 - X_STEPS[half], 8)
        return rcopy(block, block, w_send.at[w, 2, half], w_recv.at[w, 2, half], gx=who)

    def w_mate(w, k):
        who = gx if k == 3 else lax.rem(gx + 8 - X_STEPS[k], 8)
        src = weights[w][0] if k == 3 else rows_of(w, who)
        return rcopy(src, rows_of(w, who), w_fsend.at[w, k], w_frecv.at[w, k], gx=mate)

    def w_mate_arrival(w, k):
        who = mate if k == 3 else lax.rem(mate + 8 - X_STEPS[k], 8)
        dst = rows_of(w, who)
        return rcopy(dst, dst, w_fsend.at[w, k], w_frecv.at[w, k], gx=mate)

    def send_own(w, first=True, second=True):
        if first:
            w_copy(w, 0, 0).start()
            w_copy(w, 1, 1).start()
        if second:
            w_copy(w, 0, 1).start()
            w_copy(w, 1, 0).start()

    send_own(0)
    send_own(1, second=False)
    for w in range(4):
        w_mate(w, 3).start()

    def pass_weights(w):
        for half in range(2):
            w_arrival(w, half, half).wait_recv()
            w_onward(w, half).start()
        for k in range(2):
            w_arrival(w, k, 1 - k).wait_recv()
            w_mate(w, k).start()

    def last_weights(w):
        for half in range(2):
            w_onward_arrival(w, half).wait_recv()
        w_mate(w, 2).start()

    def weights_here(w):
        for k in range(4):
            w_mate_arrival(w, k).wait_recv()
        own_copy(w).wait()

    attn_all[gy] = attn_ref[...]
    attn_far_arrival().wait_recv()
    for d in range(1, 4):
        attn_onward(d).start()
    pass_weights(0)
    send_own(1, first=False)
    send_own(2)
    pl.semaphore_wait(hello, 1)

    def gain_copy():
        return rcopy(gain_ref, gain_recv, z_send.at[0], z_recv.at[0], gz=across)

    gain_copy().start()
    for d in range(1, 4):
        attn_arrival(d, False).wait_recv()
        attn_arrival(d, True).wait_recv()
    last_weights(0)

    def y_copy(n, d):
        who = lax.rem(y + d, 4)
        return rcopy(
            y_send.at[n, who], y_recv.at[n, d - 1], ys_send.at[n, d - 1], ys_recv.at[n, d - 1],
            gz=zh * 4 + who,
        )

    def keep_tiles(n, m, total):
        for half in range(2):
            block = 2 * m + half
            tile = total[:, half * TILE : (half + 1) * TILE]
            part8[block] = tile
            y_send[n, block % 4, block // 4] = tile.astype(BF16)

    def y_sum(n, side):
        total = part8[side * 4 + y]
        for d in range(3):
            total += y_recv[n, d, side].astype(F32)
        return total

    weights_here(0)
    for m in range(4):
        total = None
        for k in range(4):
            left = jnp.concatenate([attn_all[2 * k], attn_all[2 * k + 1]], axis=1)
            term = dot(left, wp[k * 256 : (k + 1) * 256, m * 256 : (m + 1) * 256])
            total = term if total is None else total + term
        keep_tiles(0, m, total)
    for d in range(1, 4):
        y_copy(0, d).start()
    pass_weights(1)
    for d in range(1, 4):
        y_copy(0, d).wait_recv()

    def zh_copy():
        return rcopy(zh_send.at[pl.ds(0, 2)], zh_recv.at[pl.ds(0, 2)], z_send.at[1], z_recv.at[1], gz=across)

    mine = res_ref[...].astype(F32) + y_sum(0, zh)
    theirs = y_sum(0, 1 - zh)
    zh_send[0] = mine.astype(BF16)
    zh_send[1] = theirs.astype(BF16)
    zh_copy().start()
    pass_weights(2)
    send_own(3)
    last_weights(1)
    gain_copy().wait_recv()
    zh_copy().wait_recv()
    mine += zh_recv[1].astype(F32)
    theirs += zh_recv[0].astype(F32)
    stream[...] = mine
    scaled[y, zh] = (mine * gain_ref[...]).astype(BF16)
    scaled[y, 1 - zh] = (theirs * gain_recv[...]).astype(BF16)

    def scaled_copy(d):
        who = zh * 4 + lax.rem(y + d, 4)
        return rcopy(scaled.at[y], scaled.at[y], ya_send.at[d], ya_recv.at[d], gz=who)

    def scaled_arrival(d):
        who = lax.rem(y + 4 - d, 4)
        return rcopy(scaled.at[who], scaled.at[who], ya_send.at[d], ya_recv.at[d], gz=zh * 4 + who)

    def ssq_copy(d):
        who = zh * 4 + lax.rem(y + d, 4)
        return rcopy(ssq_y.at[0], ssq_y.at[d], sy_send.at[d], sy_recv.at[d], gz=who)

    def ssq_gy_copy(d):
        who = lax.rem(gy + d, 8)
        return rcopy(ssq_gy.at[0], ssq_gy.at[d], sg_send.at[d], sg_recv.at[d], gy=who)

    for d in range(1, 4):
        scaled_copy(d).start()
    squares = jnp.sum(mine * mine + theirs * theirs, axis=1, keepdims=True)
    squares = jnp.concatenate(
        [jnp.broadcast_to(squares, (ROWS, TILE)), jnp.zeros((256 - ROWS, TILE), F32)], axis=0
    )
    ssq_y[0] = squares.T[:8]
    for d in range(1, 4):
        ssq_copy(d).start()
    last_weights(2)
    for d in range(1, 4):
        scaled_arrival(d).wait_recv()
        ssq_copy(d).wait_recv()
    ssq_gy[0] = (ssq_y[0] + ssq_y[1] + ssq_y[2] + ssq_y[3])[:1]
    for d in range(1, 8):
        ssq_gy_copy(d).start()

    weights_here(1)
    weights_here(2)

    def products(unit):
        columns = pl.ds(pl.multiple_of(unit * UNIT, UNIT), UNIT)
        for part, w in enumerate((wg, wu)):
            total = None
            for k in range(4):
                a, b = 2 * k, 2 * k + 1
                left = jnp.concatenate([scaled[a % 4, a // 4], scaled[b % 4, b // 4]], axis=1)
                term = dot(left, w[k * 256 : (k + 1) * 256, columns])
                total = term if total is None else total + term
            for half in range(2):
                gu[unit, 2 * part + half] = total[:, half * TILE : (half + 1) * TILE]

    def r_copy(unit, part):
        return rcopy(
            acc_r.at[unit, part], acc_r.at[unit, part], r_send.at[unit, part], r_recv.at[unit, part],
            gy=up_chip,
        )

    def l_copy(unit, part):
        return rcopy(
            acc_l.at[unit, part], acc_l.at[unit, part], l_send.at[unit, part], l_recv.at[unit, part],
            gy=down_chip,
        )

    def pass_on(tile, unit, copy, acc, first):
        @pl.when(first)
        def _():
            acc[unit, tile] = gu[unit, tile].astype(BF16)

        @pl.when(jnp.logical_not(first))
        def _():
            copy(unit, tile).wait_recv()
            acc[unit, tile] = (gu[unit, tile] + acc[unit, tile].astype(F32)).astype(BF16)

        copy(unit, tile).start()

    def owner_of(unit):
        return unit + lax.min(lax.max(unit - 3, 0), 1)

    def line_step(t, carry):
        @pl.when(t < 4)
        def _():
            products(lax.select(gy < 4, 6 - t, t))

        right, left = 6 - t + gy, t - 7 + gy
        for tile in range(4):

            @pl.when(jnp.logical_and(t >= gy, owner_of(right) > gy))
            def _():
                pass_on(tile, right, r_copy, acc_r, gy == 0)

            @pl.when(jnp.logical_and(left >= 0, owner_of(left) < gy))
            def _():
                pass_on(tile, left, l_copy, acc_l, gy == 7)

        @pl.when(t < 3)
        def _():
            products(lax.select(gy < 4, t, 6 - t))

        @pl.when(t == 2)
        def _():
            pass_weights(3)

        @pl.when(t == 5)
        def _():
            last_weights(3)

        return carry

    lax.fori_loop(0, 7, line_step, 0)

    for d in range(1, 8):
        ssq_gy_copy(d).wait_recv()
    total = ssq_gy[0]
    for d in range(1, 8):
        total += ssq_gy[d]
    total = lax.rsqrt(total / D + 1e-05)
    inv[...] = jnp.broadcast_to(total, (TILE, 256)).T

    owns = gy != 4
    own_unit = gy - lax.min(lax.max(gy - 4, 0), 1)

    @pl.when(owns)
    def _():
        for tile in range(4):

            @pl.when(gy > 0)
            def _():
                r_copy(own_unit, tile).wait_recv()
                gu[own_unit, tile] += acc_r[own_unit, tile].astype(F32)

            @pl.when(gy < 7)
            def _():
                l_copy(own_unit, tile).wait_recv()
                gu[own_unit, tile] += acc_l[own_unit, tile].astype(F32)

        for half in range(2):
            gate = inv[:ROWS] * gu[own_unit, half]
            up = inv[:ROWS] * gu[own_unit, 2 + half]
            hid[own_unit, half] = (gate / (1.0 + jnp.exp(-gate)) * up).astype(BF16)

    weights_here(3)

    def hidden_copy(unit, k, side, hop):
        half, piece = k // 2, k % 2
        block = hid.at[unit, half, pl.ds(*PIECES[piece])]
        who = lax.max(lax.min(gy + (1 - 2 * side) * hop, 7), 0)
        return rcopy(block, block, h_send.at[unit, side, hop - 1, k], h_recv.at[unit, k], gy=who)

    def hidden_sends(unit, k, side, act):
        room = (7 - gy, gy)[side]
        for hop in (2, 1):

            @pl.when(room >= hop)
            def _():
                act(hidden_copy(unit, k, side, hop))

    def add_down(unit):
        left = jnp.concatenate([hid[unit, 0], hid[unit, 1]], axis=1)
        rows = pl.ds(pl.multiple_of(unit * UNIT, UNIT), UNIT)
        for m in range(4):
            down[m] += dot(left, wd[rows, m * 256 : (m + 1) * 256])

    down[...] = jnp.zeros_like(down)

    @pl.when(owns)
    def _():
        for k in range(4):
            for side in range(2):
                hidden_sends(own_unit, k, side, lambda copy: copy.start())

        add_down(own_unit)

    def source(side, far):
        chip = gy - far if side == 0 else gy + far
        there = jnp.logical_and(jnp.logical_and(chip >= 0, chip <= 7), chip != 4)
        return there, chip - lax.min(lax.max(chip - 4, 0), 1)

    def hidden_step(t, carry):
        for k in range(4):
            for side in range(2):
                there, unit = source(side, 2 * t)

                @pl.when(there)
                def _():
                    hidden_copy(unit, k, side, 1).wait_recv()
                    hidden_sends(unit, k, side, lambda copy: copy.start())

        for side in range(2):
            there, unit = source(side, 2 * t - 1)

            @pl.when(there)
            def _():
                for k in range(4):
                    hidden_copy(unit, k, side, 1).wait_recv()
                add_down(unit)

            there, unit = source(side, 2 * t)

            @pl.when(there)
            def _():
                add_down(unit)

        return carry

    lax.fori_loop(1, 5, hidden_step, 0)

    for m in range(4):
        keep_tiles(1, m, down[m])
    for d in range(1, 4):
        y_copy(1, d).start()
    for d in range(1, 4):
        y_copy(1, d).wait_recv()

    def last_copy():
        return rcopy(zh_send.at[2], zh_recv.at[2], z_send.at[2], z_recv.at[2], gz=across)

    zh_send[2] = y_sum(1, 1 - zh).astype(BF16)
    last_copy().start()
    stream[...] += y_sum(1, zh)
    last_copy().wait_recv()
    out_ref[...] = (stream[...] + zh_recv[2].astype(F32)).astype(BF16)

    for d in range(1, 8):
        ssq_gy_copy(d).wait_send()
    attn_far().wait_send()
    for d in range(1, 4):
        attn_near(d).wait_send()
        attn_onward(d).wait_send()
    for w in range(4):
        for k in range(4):
            w_mate(w, k).wait_send()
    for w in range(4):
        for half in range(2):
            w_copy(w, 0, half).wait_send()
            w_copy(w, 1, half).wait_send()
            w_onward(w, half).wait_send()
    for d in range(1, 4):
        y_copy(0, d).wait_send()
        y_copy(1, d).wait_send()
        scaled_copy(d).wait_send()
        ssq_copy(d).wait_send()
    gain_copy().wait_send()
    zh_copy().wait_send()
    last_copy().wait_send()

    def drain(unit, carry):
        owner = owner_of(unit)
        for k in range(4):

            @pl.when(owner > gy)
            def _():
                r_copy(unit, k).wait_send()

            @pl.when(owner < gy)
            def _():
                l_copy(unit, k).wait_send()

            for side, far in ((0, gy - owner), (1, owner - gy)):

                @pl.when(jnp.logical_and(far >= 0, lax.rem(far + 8, 2) == 0))
                def _():
                    hidden_sends(unit, k, side, lambda copy: copy.wait_send())

        return carry

    lax.fori_loop(0, UNITS, drain, 0)


def on_device(attn_out, residual, proj_weight, norm_gain, gate_proj, up_proj, down_proj):
    tile = (ROWS, TILE)
    in_vmem, in_hbm = pl.BlockSpec(memory_space=pltpu.VMEM), pl.BlockSpec(memory_space=pl.ANY)
    dma = pltpu.SemaphoreType.DMA
    return pl.pallas_call(
        kernel,
        out_shape=jax.ShapeDtypeStruct(tile, BF16),
        in_specs=[in_vmem] * 3 + [in_hbm] * 4,
        out_specs=in_vmem,
        scratch_shapes=[
            pltpu.VMEM((8, *tile), BF16),
            pltpu.VMEM((1024, 1024), BF16),
            pltpu.VMEM((1024, 1792), BF16),
            pltpu.VMEM((1024, 1792), BF16),
            pltpu.VMEM((1792, 1024), BF16),
            pltpu.VMEM((8, *tile), F32),
            pltpu.VMEM((2, 4, 2, *tile), BF16),
            pltpu.VMEM((2, 3, 2, *tile), BF16),
            pltpu.VMEM((3, *tile), BF16),
            pltpu.VMEM((3, *tile), BF16),
            pltpu.VMEM((1, TILE), F32),
            pltpu.VMEM(tile, F32),
            pltpu.VMEM((4, 2, *tile), BF16),
            pltpu.VMEM((4, 8, 256), F32),
            pltpu.VMEM((8, 1, 256), F32),
            pltpu.VMEM((256, TILE), F32),
            pltpu.VMEM((UNITS, 4, *tile), F32),
            pltpu.VMEM((UNITS, 4, *tile), BF16),
            pltpu.VMEM((UNITS, 4, *tile), BF16),
            pltpu.VMEM((UNITS, 2, *tile), BF16),
            pltpu.VMEM((4, ROWS, 256), F32),
            dma((4,)), dma((4, 3, 2)), dma((4, 3, 2)), dma((4, 4)), dma((4, 4)),
            dma((7,)), dma((7,)), pltpu.SemaphoreType.REGULAR,
            dma((2, 3)), dma((2, 3)), dma((4,)), dma((4,)),
            dma((4,)), dma((4,)), dma((8,)), dma((8,)), dma((3,)), dma((3,)),
            dma((UNITS, 4)), dma((UNITS, 4)), dma((UNITS, 4)), dma((UNITS, 4)),
            dma((UNITS, 2, 2, 4)), dma((UNITS, 4)),
        ],
        compiler_params=pltpu.CompilerParams(
            collective_id=0, has_side_effects=True, vmem_limit_bytes=56 << 20
        ),
    )(attn_out, residual, norm_gain.reshape(1, TILE), proj_weight, gate_proj, up_proj, down_proj)


def solution(mesh):
    in_specs = (
        P("gx", ("gz", "gy")),
        P("gx", ("gy", "gz")),
        P(("gz", "gx"), "gy"),
        P(("gy", "gz")),
        P(("gy", "gx"), "gz"),
        P(("gy", "gx"), "gz"),
        P(("gz", "gx"), "gy"),
    )
    return jax.shard_map(
        on_device, mesh=mesh, in_specs=in_specs, out_specs=P("gx", ("gy", "gz")), check_vma=False
    )
```

```python
import jax
import jax.numpy as jnp
from jax import lax
from jax.experimental import pallas as pl
from jax.experimental.pallas import tpu as pltpu
from jax.sharding import PartitionSpec as P

MESH = pl.DeviceIdType.MESH
D = 8192
ROWS, TILE = 176, 128
UNITS, UNIT = 7, 256
F32, BF16 = jnp.float32, jnp.bfloat16
X_STEPS = (2, 6, 4)
PIECES = ((0, 96), (96, 80))


def rcopy(src, dst, send, recv, **where):
    return pltpu.make_async_remote_copy(
        src_ref=src, dst_ref=dst, send_sem=send, recv_sem=recv, device_id=where, device_id_type=MESH
    )


def signal(sem, **where):
    pl.semaphore_signal(sem, inc=1, device_id=where, device_id_type=MESH)


def dot(a, b):
    return jnp.dot(a, b, preferred_element_type=F32)


def kernel(
    attn_ref, res_ref, gain_ref, wp_hbm, wg_hbm, wu_hbm, wd_hbm, out_ref,
    attn_all, wp, wg, wu, wd, part8, y_send, y_recv, zh_send, zh_recv,
    gain_recv, stream, scaled, ssq_y, ssq_gy, inv, gu, acc_r, acc_l, hid, down,
    w_local, w_send, w_recv, w_fsend, w_frecv, a_send, a_recv, hello, ys_send, ys_recv, ya_send, ya_recv,
    sy_send, sy_recv, sg_send, sg_recv, z_send, z_recv, r_send, r_recv, l_send, l_recv,
    h_send, h_recv,
):
    gx, gy, gz = lax.axis_index("gx"), lax.axis_index("gy"), lax.axis_index("gz")
    mate = gx + 1 - 2 * lax.rem(gx, 2)
    y, zh = lax.rem(gz, 4), gz // 4
    across = lax.rem(gz + 4, 8)
    up_chip, down_chip = lax.min(gy + 1, 7), lax.max(gy - 1, 0)

    pieces = (
        (wp_hbm, wp, 0, 1024), (wg_hbm, wg, 0, 1024), (wu_hbm, wu, 0, 1024),
        (wg_hbm, wg, 1024, 768), (wu_hbm, wu, 1024, 768), (wd_hbm, wd, 0, 1024),
    )

    def own_rows(w):
        src, _, first, width = pieces[w]
        return src.at[:, pl.ds(first, width)]

    def rows_of(w, who):
        src, dst, first, width = pieces[w]
        depth = src.shape[0]
        return dst.at[pl.ds(pl.multiple_of(who * depth, 16), depth), pl.ds(first, width)]

    def own_copy(w):
        return pltpu.make_async_copy(own_rows(w), rows_of(w, gx), w_local.at[w])

    for w in range(6):
        own_copy(w).start()

    far_gy, quad, place = lax.rem(gy + 4, 8), gy // 4 * 4, lax.rem(gy, 4)

    def in_quad(d):
        return quad + lax.rem(place + d, 4)

    barrier = pltpu.get_barrier_semaphore()
    for step in X_STEPS:
        signal(barrier, gx=lax.rem(gx + step, 8))
    signal(barrier, gx=mate)
    for d in range(1, 4):
        signal(barrier, gz=zh * 4 + lax.rem(y + d, 4))
        signal(barrier, gy=in_quad(d))
    signal(barrier, gy=far_gy)
    signal(barrier, gy=far_gy, gz=across)
    pl.semaphore_wait(barrier, 12)
    signal(hello, gy=far_gy, gz=across)

    def attn_far():
        return rcopy(attn_ref, attn_all.at[gy], a_send.at[0], a_recv.at[0], gy=far_gy)

    def attn_far_arrival():
        return rcopy(attn_ref, attn_all.at[far_gy], a_send.at[0], a_recv.at[0], gy=far_gy)

    def attn_near(d):
        return rcopy(attn_ref, attn_all.at[gy], a_send.at[d], a_recv.at[d], gy=in_quad(d))

    def attn_onward(d):
        block = attn_all.at[far_gy]
        return rcopy(block, block, a_send.at[3 + d], a_recv.at[3 + d], gy=in_quad(d))

    def attn_arrival(d, onward):
        who = in_quad(4 - d)
        block = attn_all.at[lax.rem(who + 4, 8) if onward else who]
        k = d + 3 if onward else d
        return rcopy(block, block, a_send.at[k], a_recv.at[k], gy=who)

    attn_far().start()
    for d in range(1, 4):
        attn_near(d).start()

    def half_of(w, who, half):
        src, dst, first, width = pieces[w]
        depth = src.shape[0] // 2
        return dst.at[pl.ds(pl.multiple_of((2 * who + half) * depth, 16), depth), pl.ds(first, width)]

    def own_half(w, half):
        src, _, first, width = pieces[w]
        depth = src.shape[0] // 2
        return src.at[pl.ds(half * depth, depth), pl.ds(first, width)]

    def w_copy(w, k, half):
        who = lax.rem(gx + X_STEPS[k], 8)
        return rcopy(
            own_half(w, half), half_of(w, gx, half), w_send.at[w, k, half], w_recv.at[w, k, half], gx=who
        )

    def w_arrival(w, k, half):
        who = lax.rem(gx + 8 - X_STEPS[k], 8)
        dst = half_of(w, who, half)
        return rcopy(dst, dst, w_send.at[w, k, half], w_recv.at[w, k, half], gx=who)

    def w_onward(w, half):
        origin, who = lax.rem(gx + 8 - X_STEPS[half], 8), lax.rem(gx + X_STEPS[half], 8)
        block = half_of(w, origin, half)
        return rcopy(block, block, w_send.at[w, 2, half], w_recv.at[w, 2, half], gx=who)

    def w_onward_arrival(w, half):
        block = half_of(w, lax.rem(gx + 4, 8), half)
        who = lax.rem(gx + 8 - X_STEPS[half], 8)
        return rcopy(block, block, w_send.at[w, 2, half], w_recv.at[w, 2, half], gx=who)

    def w_mate(w, k):
        who = gx if k == 3 else lax.rem(gx + 8 - X_STEPS[k], 8)
        src = own_rows(w) if k == 3 else rows_of(w, who)
        return rcopy(src, rows_of(w, who), w_fsend.at[w, k], w_frecv.at[w, k], gx=mate)

    def w_mate_arrival(w, k):
        who = mate if k == 3 else lax.rem(mate + 8 - X_STEPS[k], 8)
        dst = rows_of(w, who)
        return rcopy(dst, dst, w_fsend.at[w, k], w_frecv.at[w, k], gx=mate)

    def send_own(w):
        w_copy(w, 0, 0).start()
        w_copy(w, 1, 1).start()
        w_copy(w, 0, 1).start()
        w_copy(w, 1, 0).start()

    send_own(0)
    for w in range(6):
        w_mate(w, 3).start()

    def pass_weights(w):
        for half in range(2):
            w_arrival(w, half, half).wait_recv()
            w_onward(w, half).start()
        for k in range(2):
            w_arrival(w, k, 1 - k).wait_recv()
            w_mate(w, k).start()

    def last_weights(w):
        for half in range(2):
            w_onward_arrival(w, half).wait_recv()
        w_mate(w, 2).start()

    def weights_here(w):
        for k in range(4):
            w_mate_arrival(w, k).wait_recv()
        own_copy(w).wait()

    attn_all[gy] = attn_ref[...]
    attn_far_arrival().wait_recv()
    for d in range(1, 4):
        attn_onward(d).start()
    pass_weights(0)
    send_own(1)
    send_own(2)
    pl.semaphore_wait(hello, 1)

    def gain_copy():
        return rcopy(gain_ref, gain_recv, z_send.at[0], z_recv.at[0], gz=across)

    gain_copy().start()
    for d in range(1, 4):
        attn_arrival(d, False).wait_recv()
        attn_arrival(d, True).wait_recv()
    last_weights(0)

    def y_copy(n, d):
        who = lax.rem(y + d, 4)
        return rcopy(
            y_send.at[n, who], y_recv.at[n, d - 1], ys_send.at[n, d - 1], ys_recv.at[n, d - 1],
            gz=zh * 4 + who,
        )

    def keep_tiles(n, m, total):
        for half in range(2):
            block = 2 * m + half
            tile = total[:, half * TILE : (half + 1) * TILE]
            part8[block] = tile
            y_send[n, block % 4, block // 4] = tile.astype(BF16)

    def y_sum(n, side):
        total = part8[side * 4 + y]
        for d in range(3):
            total += y_recv[n, d, side].astype(F32)
        return total

    weights_here(0)
    for m in range(4):
        total = None
        for k in range(4):
            left = jnp.concatenate([attn_all[2 * k], attn_all[2 * k + 1]], axis=1)
            term = dot(left, wp[k * 256 : (k + 1) * 256, m * 256 : (m + 1) * 256])
            total = term if total is None else total + term
        keep_tiles(0, m, total)
    for d in range(1, 4):
        y_copy(0, d).start()
    pass_weights(1)
    send_own(3)
    for d in range(1, 4):
        y_copy(0, d).wait_recv()

    def zh_copy():
        return rcopy(zh_send.at[pl.ds(0, 2)], zh_recv.at[pl.ds(0, 2)], z_send.at[1], z_recv.at[1], gz=across)

    mine = res_ref[...].astype(F32) + y_sum(0, zh)
    theirs = y_sum(0, 1 - zh)
    zh_send[0] = mine.astype(BF16)
    zh_send[1] = theirs.astype(BF16)
    zh_copy().start()
    pass_weights(2)
    send_own(4)
    last_weights(1)
    pass_weights(3)
    gain_copy().wait_recv()
    zh_copy().wait_recv()
    mine += zh_recv[1].astype(F32)
    theirs += zh_recv[0].astype(F32)
    stream[...] = mine
    scaled[y, zh] = (mine * gain_ref[...]).astype(BF16)
    scaled[y, 1 - zh] = (theirs * gain_recv[...]).astype(BF16)

    def scaled_copy(d):
        who = zh * 4 + lax.rem(y + d, 4)
        return rcopy(scaled.at[y], scaled.at[y], ya_send.at[d], ya_recv.at[d], gz=who)

    def scaled_arrival(d):
        who = lax.rem(y + 4 - d, 4)
        return rcopy(scaled.at[who], scaled.at[who], ya_send.at[d], ya_recv.at[d], gz=zh * 4 + who)

    def ssq_copy(d):
        who = zh * 4 + lax.rem(y + d, 4)
        return rcopy(ssq_y.at[0], ssq_y.at[d], sy_send.at[d], sy_recv.at[d], gz=who)

    def ssq_gy_copy(d):
        who = lax.rem(gy + d, 8)
        return rcopy(ssq_gy.at[0], ssq_gy.at[d], sg_send.at[d], sg_recv.at[d], gy=who)

    for d in range(1, 4):
        scaled_copy(d).start()
    squares = jnp.sum(mine * mine + theirs * theirs, axis=1, keepdims=True)
    squares = jnp.concatenate(
        [jnp.broadcast_to(squares, (ROWS, TILE)), jnp.zeros((256 - ROWS, TILE), F32)], axis=0
    )
    ssq_y[0] = squares.T[:8]
    for d in range(1, 4):
        ssq_copy(d).start()
    last_weights(2)
    pass_weights(4)
    send_own(5)
    for d in range(1, 4):
        scaled_arrival(d).wait_recv()
        ssq_copy(d).wait_recv()
    ssq_gy[0] = (ssq_y[0] + ssq_y[1] + ssq_y[2] + ssq_y[3])[:1]
    for d in range(1, 8):
        ssq_gy_copy(d).start()

    weights_here(1)
    weights_here(2)

    def place_of(unit):
        return unit + 2 * lax.min(lax.max(unit - 1, 0), 1) - 5 * lax.min(lax.max(unit - 4, 0), 1)

    def products(unit, parts=(0, 1)):
        columns = pl.ds(pl.multiple_of(place_of(unit) * UNIT, UNIT), UNIT)
        for part in parts:
            w = (wg, wu)[part]
            total = None
            for k in range(4):
                a, b = 2 * k, 2 * k + 1
                left = jnp.concatenate([scaled[a % 4, a // 4], scaled[b % 4, b // 4]], axis=1)
                term = dot(left, w[k * 256 : (k + 1) * 256, columns])
                total = term if total is None else total + term
            for half in range(2):
                gu[unit, 2 * part + half] = total[:, half * TILE : (half + 1) * TILE]

    def r_copy(unit, part):
        return rcopy(
            acc_r.at[unit, part], acc_r.at[unit, part], r_send.at[unit, part], r_recv.at[unit, part],
            gy=up_chip,
        )

    def l_copy(unit, part):
        return rcopy(
            acc_l.at[unit, part], acc_l.at[unit, part], l_send.at[unit, part], l_recv.at[unit, part],
            gy=down_chip,
        )

    def pass_on(tile, unit, copy, acc, first):
        @pl.when(first)
        def _():
            acc[unit, tile] = gu[unit, tile].astype(BF16)

        @pl.when(jnp.logical_not(first))
        def _():
            copy(unit, tile).wait_recv()
            acc[unit, tile] = (gu[unit, tile] + acc[unit, tile].astype(F32)).astype(BF16)

        copy(unit, tile).start()

    def owner_of(unit):
        return unit + lax.min(lax.max(unit - 3, 0), 1)

    def line_step(t, carry):
        right, left = 6 - t + gy, t - 7 + gy

        @pl.when(t == 2)
        def _():
            weights_here(3)
            weights_here(4)

        for tile in range(4):
            if tile % 2 == 0:

                @pl.when(t < 4)
                def _():
                    products(lax.select(gy < 4, 6 - t, t), (tile // 2,))

            @pl.when(jnp.logical_and(t >= gy, owner_of(right) > gy))
            def _():
                pass_on(tile, right, r_copy, acc_r, gy == 0)

            @pl.when(jnp.logical_and(left >= 0, owner_of(left) < gy))
            def _():
                pass_on(tile, left, l_copy, acc_l, gy == 7)

        @pl.when(t < 3)
        def _():
            products(lax.select(gy < 4, t, 6 - t))

        @pl.when(t == 0)
        def _():
            last_weights(3)

        @pl.when(t == 1)
        def _():
            last_weights(4)

        @pl.when(t == 3)
        def _():
            pass_weights(5)

        @pl.when(t == 5)
        def _():
            last_weights(5)

        return carry

    lax.fori_loop(0, 7, line_step, 0)

    for d in range(1, 8):
        ssq_gy_copy(d).wait_recv()
    total = ssq_gy[0]
    for d in range(1, 8):
        total += ssq_gy[d]
    total = lax.rsqrt(total / D + 1e-05)
    inv[...] = jnp.broadcast_to(total, (TILE, 256)).T

    owns = gy != 4
    own_unit = gy - lax.min(lax.max(gy - 4, 0), 1)

    @pl.when(owns)
    def _():
        for tile in range(4):

            @pl.when(gy > 0)
            def _():
                r_copy(own_unit, tile).wait_recv()
                gu[own_unit, tile] += acc_r[own_unit, tile].astype(F32)

            @pl.when(gy < 7)
            def _():
                l_copy(own_unit, tile).wait_recv()
                gu[own_unit, tile] += acc_l[own_unit, tile].astype(F32)

        for half in range(2):
            gate = inv[:ROWS] * gu[own_unit, half]
            up = inv[:ROWS] * gu[own_unit, 2 + half]
            hid[own_unit, half] = (gate / (1.0 + jnp.exp(-gate)) * up).astype(BF16)

    weights_here(5)

    def hidden_copy(unit, k, side, hop):
        half, piece = k // 2, k % 2
        block = hid.at[unit, half, pl.ds(*PIECES[piece])]
        who = lax.max(lax.min(gy + (1 - 2 * side) * hop, 7), 0)
        return rcopy(block, block, h_send.at[unit, side, hop - 1, k], h_recv.at[unit, k], gy=who)

    def hidden_sends(unit, k, side, act):
        room = (7 - gy, gy)[side]
        for hop in (2, 1):

            @pl.when(room >= hop)
            def _():
                act(hidden_copy(unit, k, side, hop))

    def add_down(unit):
        left = jnp.concatenate([hid[unit, 0], hid[unit, 1]], axis=1)
        rows = pl.ds(pl.multiple_of(place_of(unit) * UNIT, UNIT), UNIT)
        for m in range(4):
            down[m] += dot(left, wd[rows, m * 256 : (m + 1) * 256])

    down[...] = jnp.zeros_like(down)

    @pl.when(owns)
    def _():
        for k in range(4):
            for side in range(2):
                hidden_sends(own_unit, k, side, lambda copy: copy.start())

        add_down(own_unit)

    def source(side, far):
        chip = gy - far if side == 0 else gy + far
        there = jnp.logical_and(jnp.logical_and(chip >= 0, chip <= 7), chip != 4)
        return there, chip - lax.min(lax.max(chip - 4, 0), 1)

    def hidden_step(t, carry):
        for k in range(4):
            for side in range(2):
                there, unit = source(side, 2 * t)

                @pl.when(there)
                def _():
                    hidden_copy(unit, k, side, 1).wait_recv()
                    hidden_sends(unit, k, side, lambda copy: copy.start())

        for side in range(2):
            there, unit = source(side, 2 * t - 1)

            @pl.when(there)
            def _():
                for k in range(4):
                    hidden_copy(unit, k, side, 1).wait_recv()
                add_down(unit)

            there, unit = source(side, 2 * t)

            @pl.when(there)
            def _():
                add_down(unit)

        return carry

    lax.fori_loop(1, 5, hidden_step, 0)

    for m in range(4):
        keep_tiles(1, m, down[m])
    for d in range(1, 4):
        y_copy(1, d).start()
    for d in range(1, 4):
        y_copy(1, d).wait_recv()

    def last_copy():
        return rcopy(zh_send.at[2], zh_recv.at[2], z_send.at[2], z_recv.at[2], gz=across)

    zh_send[2] = y_sum(1, 1 - zh).astype(BF16)
    last_copy().start()
    stream[...] += y_sum(1, zh)
    last_copy().wait_recv()
    out_ref[...] = (stream[...] + zh_recv[2].astype(F32)).astype(BF16)

    for d in range(1, 8):
        ssq_gy_copy(d).wait_send()
    attn_far().wait_send()
    for d in range(1, 4):
        attn_near(d).wait_send()
        attn_onward(d).wait_send()
    for w in range(6):
        for k in range(4):
            w_mate(w, k).wait_send()
    for w in range(6):
        for half in range(2):
            w_copy(w, 0, half).wait_send()
            w_copy(w, 1, half).wait_send()
            w_onward(w, half).wait_send()
    for d in range(1, 4):
        y_copy(0, d).wait_send()
        y_copy(1, d).wait_send()
        scaled_copy(d).wait_send()
        ssq_copy(d).wait_send()
    gain_copy().wait_send()
    zh_copy().wait_send()
    last_copy().wait_send()

    def drain(unit, carry):
        owner = owner_of(unit)
        for k in range(4):

            @pl.when(owner > gy)
            def _():
                r_copy(unit, k).wait_send()

            @pl.when(owner < gy)
            def _():
                l_copy(unit, k).wait_send()

            for side, far in ((0, gy - owner), (1, owner - gy)):

                @pl.when(jnp.logical_and(far >= 0, lax.rem(far + 8, 2) == 0))
                def _():
                    hidden_sends(unit, k, side, lambda copy: copy.wait_send())

        return carry

    lax.fori_loop(0, UNITS, drain, 0)


def on_device(attn_out, residual, proj_weight, norm_gain, gate_proj, up_proj, down_proj):
    tile = (ROWS, TILE)
    in_vmem, in_hbm = pl.BlockSpec(memory_space=pltpu.VMEM), pl.BlockSpec(memory_space=pl.ANY)
    dma = pltpu.SemaphoreType.DMA
    return pl.pallas_call(
        kernel,
        out_shape=jax.ShapeDtypeStruct(tile, BF16),
        in_specs=[in_vmem] * 3 + [in_hbm] * 4,
        out_specs=in_vmem,
        scratch_shapes=[
            pltpu.VMEM((8, *tile), BF16),
            pltpu.VMEM((1024, 1024), BF16),
            pltpu.VMEM((1024, 1792), BF16),
            pltpu.VMEM((1024, 1792), BF16),
            pltpu.VMEM((1792, 1024), BF16),
            pltpu.VMEM((8, *tile), F32),
            pltpu.VMEM((2, 4, 2, *tile), BF16),
            pltpu.VMEM((2, 3, 2, *tile), BF16),
            pltpu.VMEM((3, *tile), BF16),
            pltpu.VMEM((3, *tile), BF16),
            pltpu.VMEM((1, TILE), F32),
            pltpu.VMEM(tile, F32),
            pltpu.VMEM((4, 2, *tile), BF16),
            pltpu.VMEM((4, 8, 256), F32),
            pltpu.VMEM((8, 1, 256), F32),
            pltpu.VMEM((256, TILE), F32),
            pltpu.VMEM((UNITS, 4, *tile), F32),
            pltpu.VMEM((UNITS, 4, *tile), BF16),
            pltpu.VMEM((UNITS, 4, *tile), BF16),
            pltpu.VMEM((UNITS, 2, *tile), BF16),
            pltpu.VMEM((4, ROWS, 256), F32),
            dma((6,)), dma((6, 3, 2)), dma((6, 3, 2)), dma((6, 4)), dma((6, 4)),
            dma((7,)), dma((7,)), pltpu.SemaphoreType.REGULAR,
            dma((2, 3)), dma((2, 3)), dma((4,)), dma((4,)),
            dma((4,)), dma((4,)), dma((8,)), dma((8,)), dma((3,)), dma((3,)),
            dma((UNITS, 4)), dma((UNITS, 4)), dma((UNITS, 4)), dma((UNITS, 4)),
            dma((UNITS, 2, 2, 4)), dma((UNITS, 4)),
        ],
        compiler_params=pltpu.CompilerParams(
            collective_id=0, has_side_effects=True, vmem_limit_bytes=56 << 20
        ),
    )(attn_out, residual, norm_gain.reshape(1, TILE), proj_weight, gate_proj, up_proj, down_proj)


def solution(mesh):
    in_specs = (
        P("gx", ("gz", "gy")),
        P("gx", ("gy", "gz")),
        P(("gz", "gx"), "gy"),
        P(("gy", "gz")),
        P(("gy", "gx"), "gz"),
        P(("gy", "gx"), "gz"),
        P(("gz", "gx"), "gy"),
    )
    return jax.shard_map(
        on_device, mesh=mesh, in_specs=in_specs, out_specs=P("gx", ("gy", "gz")), check_vma=False
    )
```

```python
import jax
import jax.numpy as jnp
from jax import lax
from jax.experimental import pallas as pl
from jax.experimental.pallas import tpu as pltpu
from jax.sharding import PartitionSpec as P

MESH = pl.DeviceIdType.MESH
D = 8192
ROWS, TILE = 176, 128
UNITS, UNIT = 7, 256
F32, BF16 = jnp.float32, jnp.bfloat16
X_STEPS = (2, 6, 4)
PIECES = ((0, 96), (96, 80))
PARTS = ((0, 64), (64, 64), (128, 48))


def rcopy(src, dst, send, recv, **where):
    return pltpu.make_async_remote_copy(
        src_ref=src, dst_ref=dst, send_sem=send, recv_sem=recv, device_id=where, device_id_type=MESH
    )


def signal(sem, **where):
    pl.semaphore_signal(sem, inc=1, device_id=where, device_id_type=MESH)


def dot(a, b):
    return jnp.dot(a, b, preferred_element_type=F32)


def kernel(
    attn_ref, res_ref, gain_ref, wp_hbm, wg_hbm, wu_hbm, wd_hbm, out_ref,
    attn_all, wp, wg, wu, wd, part8, y_send, y_recv, zh_send, zh_recv,
    gain_recv, stream, other, scaled, ssq_y, ssq_gy, inv, gu, acc_r, acc_l, hid, down,
    w_local, w_send, w_recv, w_fsend, w_frecv, a_send, a_recv, hello, ys_send, ys_recv, ya_send, ya_recv,
    sy_send, sy_recv, sg_send, sg_recv, z_send, z_recv, r_send, r_recv, l_send, l_recv,
    h_send, h_recv,
):
    gx, gy, gz = lax.axis_index("gx"), lax.axis_index("gy"), lax.axis_index("gz")
    mate = gx + 1 - 2 * lax.rem(gx, 2)
    y, zh = lax.rem(gz, 4), gz // 4
    across = lax.rem(gz + 4, 8)
    up_chip, down_chip = lax.min(gy + 1, 7), lax.max(gy - 1, 0)

    pieces = (
        (wp_hbm, wp, 0, 1024), (wg_hbm, wg, 0, 1024), (wu_hbm, wu, 0, 1024),
        (wg_hbm, wg, 1024, 768), (wu_hbm, wu, 1024, 768), (wd_hbm, wd, 0, 1024),
    )

    def own_rows(w):
        src, _, first, width = pieces[w]
        return src.at[:, pl.ds(first, width)]

    def rows_of(w, who):
        src, dst, first, width = pieces[w]
        depth = src.shape[0]
        return dst.at[pl.ds(pl.multiple_of(who * depth, 16), depth), pl.ds(first, width)]

    def own_copy(w):
        return pltpu.make_async_copy(own_rows(w), rows_of(w, gx), w_local.at[w])

    for w in range(6):
        own_copy(w).start()

    far_gy, quad, place = lax.rem(gy + 4, 8), gy // 4 * 4, lax.rem(gy, 4)

    def in_quad(d):
        return quad + lax.rem(place + d, 4)

    barrier = pltpu.get_barrier_semaphore()
    for step in X_STEPS:
        signal(barrier, gx=lax.rem(gx + step, 8))
    signal(barrier, gx=mate)
    for d in range(1, 4):
        signal(barrier, gz=zh * 4 + lax.rem(y + d, 4))
        signal(barrier, gy=in_quad(d))
    signal(barrier, gy=far_gy)
    signal(barrier, gy=far_gy, gz=across)
    pl.semaphore_wait(barrier, 12)
    signal(hello, gy=far_gy, gz=across)
    for w in range(6):
        own_copy(w).wait()

    def attn_far():
        return rcopy(attn_ref, attn_all.at[gy], a_send.at[0], a_recv.at[0], gy=far_gy)

    def attn_far_arrival():
        return rcopy(attn_ref, attn_all.at[far_gy], a_send.at[0], a_recv.at[0], gy=far_gy)

    def attn_near(d):
        return rcopy(attn_ref, attn_all.at[gy], a_send.at[d], a_recv.at[d], gy=in_quad(d))

    def attn_onward(d):
        block = attn_all.at[far_gy]
        return rcopy(block, block, a_send.at[3 + d], a_recv.at[3 + d], gy=in_quad(d))

    def attn_arrival(d, onward):
        who = in_quad(4 - d)
        block = attn_all.at[lax.rem(who + 4, 8) if onward else who]
        k = d + 3 if onward else d
        return rcopy(block, block, a_send.at[k], a_recv.at[k], gy=who)

    attn_far().start()
    for d in range(1, 4):
        attn_near(d).start()

    def half_of(w, who, half):
        src, dst, first, width = pieces[w]
        depth = src.shape[0] // 2
        return dst.at[pl.ds(pl.multiple_of((2 * who + half) * depth, 16), depth), pl.ds(first, width)]

    def w_copy(w, k, half):
        who = lax.rem(gx + X_STEPS[k], 8)
        return rcopy(
            half_of(w, gx, half), half_of(w, gx, half), w_send.at[w, k, half], w_recv.at[w, k, half], gx=who
        )

    def w_arrival(w, k, half):
        who = lax.rem(gx + 8 - X_STEPS[k], 8)
        dst = half_of(w, who, half)
        return rcopy(dst, dst, w_send.at[w, k, half], w_recv.at[w, k, half], gx=who)

    def w_onward(w, half):
        origin, who = lax.rem(gx + 8 - X_STEPS[half], 8), lax.rem(gx + X_STEPS[half], 8)
        block = half_of(w, origin, half)
        return rcopy(block, block, w_send.at[w, 2, half], w_recv.at[w, 2, half], gx=who)

    def w_onward_arrival(w, half):
        block = half_of(w, lax.rem(gx + 4, 8), half)
        who = lax.rem(gx + 8 - X_STEPS[half], 8)
        return rcopy(block, block, w_send.at[w, 2, half], w_recv.at[w, 2, half], gx=who)

    def w_mate(w, k):
        who = gx if k == 3 else lax.rem(gx + 8 - X_STEPS[k], 8)
        return rcopy(rows_of(w, who), rows_of(w, who), w_fsend.at[w, k], w_frecv.at[w, k], gx=mate)

    def w_mate_arrival(w, k):
        who = mate if k == 3 else lax.rem(mate + 8 - X_STEPS[k], 8)
        dst = rows_of(w, who)
        return rcopy(dst, dst, w_fsend.at[w, k], w_frecv.at[w, k], gx=mate)

    def send_own(w):
        w_copy(w, 0, 0).start()
        w_copy(w, 1, 1).start()
        w_copy(w, 0, 1).start()
        w_copy(w, 1, 0).start()

    send_own(0)
    for w in range(6):
        w_mate(w, 3).start()

    def pass_onward(w):
        for half in range(2):
            w_arrival(w, half, half).wait_recv()
            w_onward(w, half).start()

    def pass_to_mate(w):
        for k in range(2):
            w_arrival(w, k, 1 - k).wait_recv()
            w_mate(w, k).start()

    def pass_weights(w):
        pass_onward(w)
        pass_to_mate(w)

    def last_weights(w):
        for half in range(2):
            w_onward_arrival(w, half).wait_recv()
        w_mate(w, 2).start()

    def weights_here(w):
        for k in range(4):
            w_mate_arrival(w, k).wait_recv()

    attn_all[gy] = attn_ref[...]
    pass_onward(0)
    send_own(1)
    send_own(2)
    attn_far_arrival().wait_recv()
    for d in range(1, 4):
        attn_onward(d).start()
    pass_to_mate(0)
    pl.semaphore_wait(hello, 1)

    def gain_copy():
        return rcopy(gain_ref, gain_recv, z_send.at[0, 0], z_recv.at[0, 0], gz=across)

    gain_copy().start()
    for d in range(1, 4):
        attn_arrival(d, False).wait_recv()
        attn_arrival(d, True).wait_recv()
    last_weights(0)

    def y_copy(n, d, p):
        who, rows = lax.rem(y + d, 4), pl.ds(*PARTS[p])
        return rcopy(
            y_send.at[n, who, :, rows], y_recv.at[n, d - 1, :, rows],
            ys_send.at[n, d - 1, p], ys_recv.at[n, d - 1, p], gz=zh * 4 + who,
        )

    def keep_tiles(n, m, rows, total):
        for half in range(2):
            block = 2 * m + half
            tile = total[:, half * TILE : (half + 1) * TILE]
            part8[block, rows] = tile
            y_send[n, block % 4, block // 4, rows] = tile.astype(BF16)

    def y_sum(n, side, rows):
        total = part8[side * 4 + y, rows]
        for d in range(3):
            total += y_recv[n, d, side, rows].astype(F32)
        return total

    weights_here(0)
    for p, part in enumerate(PARTS):
        rows = pl.ds(*part)
        for m in range(4):
            total = None
            for k in range(4):
                left = jnp.concatenate([attn_all[2 * k, rows], attn_all[2 * k + 1, rows]], axis=1)
                term = dot(left, wp[k * 256 : (k + 1) * 256, m * 256 : (m + 1) * 256])
                total = term if total is None else total + term
            keep_tiles(0, m, rows, total)
        for d in range(1, 4):
            y_copy(0, d, p).start()
    pass_weights(1)
    send_own(3)

    def zh_copy(p):
        rows = (pl.ds(0, 2), pl.ds(*PARTS[p]))
        return rcopy(zh_send.at[rows], zh_recv.at[rows], z_send.at[1, p], z_recv.at[1, p], gz=across)

    for p, part in enumerate(PARTS):
        rows = pl.ds(*part)
        for d in range(1, 4):
            y_copy(0, d, p).wait_recv()
        mine = res_ref[rows].astype(F32) + y_sum(0, zh, rows)
        theirs = y_sum(0, 1 - zh, rows)
        stream[rows], other[rows] = mine, theirs
        zh_send[0, rows] = mine.astype(BF16)
        zh_send[1, rows] = theirs.astype(BF16)
        zh_copy(p).start()
    pass_weights(2)
    send_own(4)
    last_weights(1)
    pass_weights(3)
    gain_copy().wait_recv()

    def scaled_copy(d, p):
        who, block = zh * 4 + lax.rem(y + d, 4), scaled.at[y, :, pl.ds(*PARTS[p])]
        return rcopy(block, block, ya_send.at[d, p], ya_recv.at[d, p], gz=who)

    def scaled_arrival(d, p):
        who = lax.rem(y + 4 - d, 4)
        block = scaled.at[who, :, pl.ds(*PARTS[p])]
        return rcopy(block, block, ya_send.at[d, p], ya_recv.at[d, p], gz=zh * 4 + who)

    def ssq_copy(d):
        who = zh * 4 + lax.rem(y + d, 4)
        return rcopy(ssq_y.at[0], ssq_y.at[d], sy_send.at[d], sy_recv.at[d], gz=who)

    def ssq_gy_copy(d):
        who = lax.rem(gy + d, 8)
        return rcopy(ssq_gy.at[0], ssq_gy.at[d], sg_send.at[d], sg_recv.at[d], gy=who)

    for p, part in enumerate(PARTS):
        rows = pl.ds(*part)
        zh_copy(p).wait_recv()
        mine = stream[rows] + zh_recv[1, rows].astype(F32)
        theirs = other[rows] + zh_recv[0, rows].astype(F32)
        stream[rows], other[rows] = mine, theirs
        scaled[y, zh, rows] = (mine * gain_ref[...]).astype(BF16)
        scaled[y, 1 - zh, rows] = (theirs * gain_recv[...]).astype(BF16)
        for d in range(1, 4):
            scaled_copy(d, p).start()
    mine, theirs = stream[...], other[...]
    squares = jnp.sum(mine * mine + theirs * theirs, axis=1, keepdims=True)
    squares = jnp.concatenate(
        [jnp.broadcast_to(squares, (ROWS, TILE)), jnp.zeros((256 - ROWS, TILE), F32)], axis=0
    )
    ssq_y[0] = squares.T[:8]
    for d in range(1, 4):
        ssq_copy(d).start()
    last_weights(2)
    pass_weights(4)
    send_own(5)
    for d in range(1, 4):
        for p in range(len(PARTS)):
            scaled_arrival(d, p).wait_recv()
        ssq_copy(d).wait_recv()
    ssq_gy[0] = (ssq_y[0] + ssq_y[1] + ssq_y[2] + ssq_y[3])[:1]
    for d in range(1, 8):
        ssq_gy_copy(d).start()

    weights_here(1)
    weights_here(2)

    def place_of(unit):
        return unit + 2 * lax.min(lax.max(unit - 1, 0), 1) - 5 * lax.min(lax.max(unit - 4, 0), 1)

    def products(unit, parts=(0, 1)):
        columns = pl.ds(pl.multiple_of(place_of(unit) * UNIT, UNIT), UNIT)
        for part in parts:
            w = (wg, wu)[part]
            total = None
            for k in range(4):
                a, b = 2 * k, 2 * k + 1
                left = jnp.concatenate([scaled[a % 4, a // 4], scaled[b % 4, b // 4]], axis=1)
                term = dot(left, w[k * 256 : (k + 1) * 256, columns])
                total = term if total is None else total + term
            for half in range(2):
                gu[unit, 2 * half + part] = total[:, half * TILE : (half + 1) * TILE]

    def r_copy(unit, part):
        return rcopy(
            acc_r.at[unit, part], acc_r.at[unit, part], r_send.at[unit, part], r_recv.at[unit, part],
            gy=up_chip,
        )

    def l_copy(unit, part):
        return rcopy(
            acc_l.at[unit, part], acc_l.at[unit, part], l_send.at[unit, part], l_recv.at[unit, part],
            gy=down_chip,
        )

    def pass_on(tile, unit, copy, acc, first):
        @pl.when(first)
        def _():
            acc[unit, tile] = gu[unit, tile].astype(BF16)

        @pl.when(jnp.logical_not(first))
        def _():
            copy(unit, tile).wait_recv()
            acc[unit, tile] = (gu[unit, tile] + acc[unit, tile].astype(F32)).astype(BF16)

        copy(unit, tile).start()

    def owner_of(unit):
        return unit + lax.min(lax.max(unit - 3, 0), 1)

    def line_step(t, carry):
        right, left = 6 - t + gy, t - 7 + gy

        @pl.when(t == 2)
        def _():
            weights_here(3)
            weights_here(4)

        for tile in range(4):
            if tile == 0:

                @pl.when(t < 4)
                def _():
                    products(lax.select(gy < 4, 6 - t, t))

            @pl.when(jnp.logical_and(t >= gy, owner_of(right) > gy))
            def _():
                pass_on(tile, right, r_copy, acc_r, gy == 0)

            @pl.when(jnp.logical_and(left >= 0, owner_of(left) < gy))
            def _():
                pass_on(tile, left, l_copy, acc_l, gy == 7)

        @pl.when(t < 3)
        def _():
            products(lax.select(gy < 4, t, 6 - t))

        @pl.when(t == 0)
        def _():
            last_weights(3)

        @pl.when(t == 1)
        def _():
            last_weights(4)

        @pl.when(t == 3)
        def _():
            pass_weights(5)

        @pl.when(t == 5)
        def _():
            last_weights(5)

        return carry

    lax.fori_loop(0, 7, line_step, 0)

    for d in range(1, 8):
        ssq_gy_copy(d).wait_recv()
    total = ssq_gy[0]
    for d in range(1, 8):
        total += ssq_gy[d]
    total = lax.rsqrt(total / D + 1e-05)
    inv[...] = jnp.broadcast_to(total, (TILE, 256)).T

    owns = gy != 4
    own_unit = gy - lax.min(lax.max(gy - 4, 0), 1)

    weights_here(5)

    def hidden_copy(unit, k, side, hop):
        half, piece = k // 2, k % 2
        block = hid.at[unit, half, pl.ds(*PIECES[piece])]
        who = lax.max(lax.min(gy + (1 - 2 * side) * hop, 7), 0)
        return rcopy(block, block, h_send.at[unit, side, hop - 1, k], h_recv.at[unit, k], gy=who)

    def hidden_sends(unit, k, side, act):
        room = (7 - gy, gy)[side]
        for hop in (2, 1):

            @pl.when(room >= hop)
            def _():
                act(hidden_copy(unit, k, side, hop))

    def add_down(unit):
        left = jnp.concatenate([hid[unit, 0], hid[unit, 1]], axis=1)
        rows = pl.ds(pl.multiple_of(place_of(unit) * UNIT, UNIT), UNIT)
        for m in range(4):
            down[m] += dot(left, wd[rows, m * 256 : (m + 1) * 256])

    down[...] = jnp.zeros_like(down)

    @pl.when(owns)
    def _():
        for half in range(2):
            for tile in (2 * half, 2 * half + 1):

                @pl.when(gy > 0)
                def _():
                    r_copy(own_unit, tile).wait_recv()
                    gu[own_unit, tile] += acc_r[own_unit, tile].astype(F32)

                @pl.when(gy < 7)
                def _():
                    l_copy(own_unit, tile).wait_recv()
                    gu[own_unit, tile] += acc_l[own_unit, tile].astype(F32)

            gate = inv[:ROWS] * gu[own_unit, 2 * half]
            up = inv[:ROWS] * gu[own_unit, 2 * half + 1]
            hid[own_unit, half] = (gate / (1.0 + jnp.exp(-gate)) * up).astype(BF16)
            for k in (2 * half, 2 * half + 1):
                for side in range(2):
                    hidden_sends(own_unit, k, side, lambda copy: copy.start())

        add_down(own_unit)

    def source(side, far):
        chip = gy - far if side == 0 else gy + far
        there = jnp.logical_and(jnp.logical_and(chip >= 0, chip <= 7), chip != 4)
        return there, chip - lax.min(lax.max(chip - 4, 0), 1)

    def hidden_step(t, carry):
        for k in range(4):
            for side in range(2):
                there, unit = source(side, 2 * t)

                @pl.when(there)
                def _():
                    hidden_copy(unit, k, side, 1).wait_recv()
                    hidden_sends(unit, k, side, lambda copy: copy.start())

        for side in range(2):
            there, unit = source(side, 2 * t - 1)

            @pl.when(there)
            def _():
                for k in range(4):
                    hidden_copy(unit, k, side, 1).wait_recv()
                add_down(unit)

            there, unit = source(side, 2 * t)

            @pl.when(there)
            def _():
                add_down(unit)

        return carry

    lax.fori_loop(1, 5, hidden_step, 0)

    def last_copy(p):
        rows = pl.ds(*PARTS[p])
        return rcopy(zh_send.at[2, rows], zh_recv.at[2, rows], z_send.at[2, p], z_recv.at[2, p], gz=across)

    for p, part in enumerate(PARTS):
        rows = pl.ds(*part)
        for m in range(4):
            keep_tiles(1, m, rows, down[m, rows])
        for d in range(1, 4):
            y_copy(1, d, p).start()
    for p, part in enumerate(PARTS):
        rows = pl.ds(*part)
        for d in range(1, 4):
            y_copy(1, d, p).wait_recv()
        zh_send[2, rows] = y_sum(1, 1 - zh, rows).astype(BF16)
        last_copy(p).start()
        stream[rows] += y_sum(1, zh, rows)
    for d in range(1, 8):
        ssq_gy_copy(d).wait_send()
    attn_far().wait_send()
    for d in range(1, 4):
        attn_near(d).wait_send()
        attn_onward(d).wait_send()
    for w in range(6):
        for k in range(4):
            w_mate(w, k).wait_send()
    for w in range(6):
        for half in range(2):
            w_copy(w, 0, half).wait_send()
            w_copy(w, 1, half).wait_send()
            w_onward(w, half).wait_send()
    for d in range(1, 4):
        for p in range(len(PARTS)):
            y_copy(0, d, p).wait_send()
            scaled_copy(d, p).wait_send()
        ssq_copy(d).wait_send()
    gain_copy().wait_send()
    for p in range(len(PARTS)):
        zh_copy(p).wait_send()

    def drain(unit, carry):
        owner = owner_of(unit)
        for k in range(4):

            @pl.when(owner > gy)
            def _():
                r_copy(unit, k).wait_send()

            @pl.when(owner < gy)
            def _():
                l_copy(unit, k).wait_send()

            for side, far in ((0, gy - owner), (1, owner - gy)):

                @pl.when(jnp.logical_and(far >= 0, lax.rem(far + 8, 2) == 0))
                def _():
                    hidden_sends(unit, k, side, lambda copy: copy.wait_send())

        return carry

    lax.fori_loop(0, UNITS, drain, 0)

    for p, part in enumerate(PARTS):
        rows = pl.ds(*part)
        last_copy(p).wait_recv()
        out_ref[rows] = (stream[rows] + zh_recv[2, rows].astype(F32)).astype(BF16)
    for p in range(len(PARTS)):
        last_copy(p).wait_send()
        for d in range(1, 4):
            y_copy(1, d, p).wait_send()


def on_device(attn_out, residual, proj_weight, norm_gain, gate_proj, up_proj, down_proj):
    tile = (ROWS, TILE)
    in_vmem, in_hbm = pl.BlockSpec(memory_space=pltpu.VMEM), pl.BlockSpec(memory_space=pl.ANY)
    dma = pltpu.SemaphoreType.DMA
    return pl.pallas_call(
        kernel,
        out_shape=jax.ShapeDtypeStruct(tile, BF16),
        in_specs=[in_vmem] * 3 + [in_hbm] * 4,
        out_specs=in_vmem,
        scratch_shapes=[
            pltpu.VMEM((8, *tile), BF16),
            pltpu.VMEM((1024, 1024), BF16),
            pltpu.VMEM((1024, 1792), BF16),
            pltpu.VMEM((1024, 1792), BF16),
            pltpu.VMEM((1792, 1024), BF16),
            pltpu.VMEM((8, *tile), F32),
            pltpu.VMEM((2, 4, 2, *tile), BF16),
            pltpu.VMEM((2, 3, 2, *tile), BF16),
            pltpu.VMEM((3, *tile), BF16),
            pltpu.VMEM((3, *tile), BF16),
            pltpu.VMEM((1, TILE), F32),
            pltpu.VMEM(tile, F32),
            pltpu.VMEM(tile, F32),
            pltpu.VMEM((4, 2, *tile), BF16),
            pltpu.VMEM((4, 8, 256), F32),
            pltpu.VMEM((8, 1, 256), F32),
            pltpu.VMEM((256, TILE), F32),
            pltpu.VMEM((UNITS, 4, *tile), F32),
            pltpu.VMEM((UNITS, 4, *tile), BF16),
            pltpu.VMEM((UNITS, 4, *tile), BF16),
            pltpu.VMEM((UNITS, 2, *tile), BF16),
            pltpu.VMEM((4, ROWS, 256), F32),
            dma((6,)), dma((6, 3, 2)), dma((6, 3, 2)), dma((6, 4)), dma((6, 4)),
            dma((7,)), dma((7,)), pltpu.SemaphoreType.REGULAR,
            dma((2, 3, len(PARTS))), dma((2, 3, len(PARTS))), dma((4, len(PARTS))), dma((4, len(PARTS))),
            dma((4,)), dma((4,)), dma((8,)), dma((8,)), dma((3, len(PARTS))), dma((3, len(PARTS))),
            dma((UNITS, 4)), dma((UNITS, 4)), dma((UNITS, 4)), dma((UNITS, 4)),
            dma((UNITS, 2, 2, 4)), dma((UNITS, 4)),
        ],
        compiler_params=pltpu.CompilerParams(
            collective_id=0, has_side_effects=True, vmem_limit_bytes=56 << 20
        ),
    )(attn_out, residual, norm_gain.reshape(1, TILE), proj_weight, gate_proj, up_proj, down_proj)


def solution(mesh):
    in_specs = (
        P("gx", ("gz", "gy")),
        P("gx", ("gy", "gz")),
        P(("gz", "gx"), "gy"),
        P(("gy", "gz")),
        P(("gy", "gx"), "gz"),
        P(("gy", "gx"), "gz"),
        P(("gz", "gx"), "gy"),
    )
    return jax.shard_map(
        on_device, mesh=mesh, in_specs=in_specs, out_specs=P("gx", ("gy", "gz")), check_vma=False
    )
```

```python
import jax
import jax.numpy as jnp
from jax import lax
from jax.experimental import pallas as pl
from jax.experimental.pallas import tpu as pltpu
from jax.sharding import PartitionSpec as P

MESH = pl.DeviceIdType.MESH
D = 8192
ROWS, TILE = 176, 128
UNITS, UNIT = 7, 256
F32, BF16 = jnp.float32, jnp.bfloat16
X_STEPS = (2, 6, 4)
PIECES = ((0, 96), (96, 80))
PARTS = ((0, 64), (64, 64), (128, 48))


def rcopy(src, dst, send, recv, **where):
    return pltpu.make_async_remote_copy(
        src_ref=src, dst_ref=dst, send_sem=send, recv_sem=recv, device_id=where, device_id_type=MESH
    )


def signal(sem, **where):
    pl.semaphore_signal(sem, inc=1, device_id=where, device_id_type=MESH)


def dot(a, b):
    return jnp.dot(a, b, preferred_element_type=F32)


def kernel(
    attn_hbm, res_hbm, gain_hbm, wp_hbm, wg_hbm, wu_hbm, wd_hbm, out_ref,
    attn_all, res_ref, gain_ref, wp, wg, wu, wd, part8, y_send, y_recv, zh_send, zh_recv,
    gain_recv, stream, other, scaled, ssq_y, ssq_gy, inv, gu, acc_r, acc_l, hid, down,
    w_local, w_send, w_recv, w_fsend, w_frecv, a_send, a_recv, f_send, f_recv, hello, ys_send, ys_recv, ya_send, ya_recv,
    sy_send, sy_recv, sg_send, sg_recv, z_send, z_recv, r_send, r_recv, l_send, l_recv,
    h_send, h_recv,
):
    gx, gy, gz = lax.axis_index("gx"), lax.axis_index("gy"), lax.axis_index("gz")
    mate = gx + 1 - 2 * lax.rem(gx, 2)
    y, zh = lax.rem(gz, 4), gz // 4
    across = lax.rem(gz + 4, 8)
    up_chip, down_chip = lax.min(gy + 1, 7), lax.max(gy - 1, 0)

    pieces = (
        (wp_hbm, wp, 0, 1024), (wg_hbm, wg, 0, 1024), (wu_hbm, wu, 0, 1024),
        (wg_hbm, wg, 1024, 768), (wu_hbm, wu, 1024, 768), (wd_hbm, wd, 0, 1024),
    )

    def own_rows(w):
        src, _, first, width = pieces[w]
        return src.at[:, pl.ds(first, width)]

    def rows_of(w, who):
        src, dst, first, width = pieces[w]
        depth = src.shape[0]
        return dst.at[pl.ds(pl.multiple_of(who * depth, 16), depth), pl.ds(first, width)]

    def own_copy(w):
        return pltpu.make_async_copy(own_rows(w), rows_of(w, gx), w_local.at[w])

    def local(k):
        src, dst = ((attn_hbm, attn_all.at[gy]), (res_hbm, res_ref), (gain_hbm, gain_ref))[k]
        return pltpu.make_async_copy(src, dst, w_local.at[6 + k])

    far_gy, quad, place = lax.rem(gy + 4, 8), gy // 4 * 4, lax.rem(gy, 4)

    def in_quad(d):
        return quad + lax.rem(place + d, 4)

    barrier = pltpu.get_barrier_semaphore()
    for step in X_STEPS:
        signal(barrier, gx=lax.rem(gx + step, 8))
    signal(barrier, gx=mate)
    for d in range(1, 4):
        signal(barrier, gz=zh * 4 + lax.rem(y + d, 4))
        signal(barrier, gy=in_quad(d))
    signal(barrier, gy=far_gy)
    signal(barrier, gy=far_gy, gz=across)
    for k in range(3):
        local(k).start()
    for w in range(6):
        own_copy(w).start()
    for k in range(3):
        local(k).wait()
    pl.semaphore_wait(barrier, 12)
    signal(hello, gy=far_gy, gz=across)
    for w in range(6):
        own_copy(w).wait()

    def attn_far(p):
        rows = pl.ds(*PIECES[p])
        return rcopy(attn_all.at[gy, rows], attn_all.at[gy, rows], f_send.at[0, p], f_recv.at[0, p], gy=far_gy)

    def attn_far_arrival(p):
        rows = pl.ds(*PIECES[p])
        return rcopy(attn_all.at[far_gy, rows], attn_all.at[far_gy, rows], f_send.at[0, p], f_recv.at[0, p], gy=far_gy)

    def attn_near(d):
        return rcopy(attn_all.at[gy], attn_all.at[gy], a_send.at[d], a_recv.at[d], gy=in_quad(d))

    def attn_onward(d, p):
        block = attn_all.at[far_gy, pl.ds(*PIECES[p])]
        return rcopy(block, block, f_send.at[d, p], f_recv.at[d, p], gy=in_quad(d))

    def attn_arrival(d):
        who = in_quad(4 - d)
        block = attn_all.at[who]
        return rcopy(block, block, a_send.at[d], a_recv.at[d], gy=who)

    def attn_onward_arrival(d, p):
        who = in_quad(4 - d)
        block = attn_all.at[lax.rem(who + 4, 8), pl.ds(*PIECES[p])]
        return rcopy(block, block, f_send.at[d, p], f_recv.at[d, p], gy=who)

    for p in range(2):
        attn_far(p).start()
    for d in range(1, 4):
        attn_near(d).start()

    def half_of(w, who, half):
        src, dst, first, width = pieces[w]
        depth = src.shape[0] // 2
        return dst.at[pl.ds(pl.multiple_of((2 * who + half) * depth, 16), depth), pl.ds(first, width)]

    def w_copy(w, k, half):
        who = lax.rem(gx + X_STEPS[k], 8)
        return rcopy(
            half_of(w, gx, half), half_of(w, gx, half), w_send.at[w, k, half], w_recv.at[w, k, half], gx=who
        )

    def w_arrival(w, k, half):
        who = lax.rem(gx + 8 - X_STEPS[k], 8)
        dst = half_of(w, who, half)
        return rcopy(dst, dst, w_send.at[w, k, half], w_recv.at[w, k, half], gx=who)

    def w_onward(w, half):
        origin, who = lax.rem(gx + 8 - X_STEPS[half], 8), lax.rem(gx + X_STEPS[half], 8)
        block = half_of(w, origin, half)
        return rcopy(block, block, w_send.at[w, 2, half], w_recv.at[w, 2, half], gx=who)

    def w_onward_arrival(w, half):
        block = half_of(w, lax.rem(gx + 4, 8), half)
        who = lax.rem(gx + 8 - X_STEPS[half], 8)
        return rcopy(block, block, w_send.at[w, 2, half], w_recv.at[w, 2, half], gx=who)

    def w_mate(w, k):
        who = gx if k == 3 else lax.rem(gx + 8 - X_STEPS[k], 8)
        return rcopy(rows_of(w, who), rows_of(w, who), w_fsend.at[w, k], w_frecv.at[w, k], gx=mate)

    def w_mate_arrival(w, k):
        who = mate if k == 3 else lax.rem(mate + 8 - X_STEPS[k], 8)
        dst = rows_of(w, who)
        return rcopy(dst, dst, w_fsend.at[w, k], w_frecv.at[w, k], gx=mate)

    def send_own(w):
        w_copy(w, 0, 0).start()
        w_copy(w, 1, 1).start()
        w_copy(w, 0, 1).start()
        w_copy(w, 1, 0).start()

    send_own(0)
    for w in range(6):
        w_mate(w, 3).start()

    def pass_onward(w):
        for half in range(2):
            w_arrival(w, half, half).wait_recv()
            w_onward(w, half).start()

    def pass_to_mate(w):
        for k in range(2):
            w_arrival(w, k, 1 - k).wait_recv()
            w_mate(w, k).start()

    def pass_weights(w):
        pass_onward(w)
        pass_to_mate(w)

    def last_weights(w):
        for half in range(2):
            w_onward_arrival(w, half).wait_recv()
        w_mate(w, 2).start()

    def weights_here(w):
        for k in range(4):
            w_mate_arrival(w, k).wait_recv()

    pass_onward(0)
    send_own(1)
    send_own(2)
    for p in range(2):
        attn_far_arrival(p).wait_recv()
        for d in range(1, 4):
            attn_onward(d, p).start()
    pass_to_mate(0)
    pl.semaphore_wait(hello, 1)

    def gain_copy():
        return rcopy(gain_ref, gain_recv, z_send.at[0, 0], z_recv.at[0, 0], gz=across)

    gain_copy().start()
    for d in range(1, 4):
        attn_arrival(d).wait_recv()
        for p in range(2):
            attn_onward_arrival(d, p).wait_recv()
    last_weights(0)

    def y_copy(n, d, p):
        who, rows = lax.rem(y + d, 4), pl.ds(*PARTS[p])
        return rcopy(
            y_send.at[n, who, :, rows], y_recv.at[n, d - 1, :, rows],
            ys_send.at[n, d - 1, p], ys_recv.at[n, d - 1, p], gz=zh * 4 + who,
        )

    def keep_tiles(n, m, rows, total):
        for half in range(2):
            block = 2 * m + half
            tile = total[:, half * TILE : (half + 1) * TILE]
            part8[block, rows] = tile
            y_send[n, block % 4, block // 4, rows] = tile.astype(BF16)

    def y_sum(n, side, rows):
        total = part8[side * 4 + y, rows]
        for d in range(3):
            total += y_recv[n, d, side, rows].astype(F32)
        return total

    weights_here(0)
    for p, part in enumerate(PARTS):
        rows = pl.ds(*part)
        for m in range(4):
            total = None
            for k in range(4):
                left = jnp.concatenate([attn_all[2 * k, rows], attn_all[2 * k + 1, rows]], axis=1)
                term = dot(left, wp[k * 256 : (k + 1) * 256, m * 256 : (m + 1) * 256])
                total = term if total is None else total + term
            keep_tiles(0, m, rows, total)
        for d in range(1, 4):
            y_copy(0, d, p).start()
    pass_weights(1)
    send_own(3)

    def zh_copy(p):
        rows = (pl.ds(0, 2), pl.ds(*PARTS[p]))
        return rcopy(zh_send.at[rows], zh_recv.at[rows], z_send.at[1, p], z_recv.at[1, p], gz=across)

    for p, part in enumerate(PARTS):
        rows = pl.ds(*part)
        for d in range(1, 4):
            y_copy(0, d, p).wait_recv()
        mine = res_ref[rows].astype(F32) + y_sum(0, zh, rows)
        theirs = y_sum(0, 1 - zh, rows)
        stream[rows], other[rows] = mine, theirs
        zh_send[0, rows] = mine.astype(BF16)
        zh_send[1, rows] = theirs.astype(BF16)
        zh_copy(p).start()
    pass_weights(2)
    send_own(4)
    last_weights(1)
    pass_weights(3)
    gain_copy().wait_recv()

    def scaled_copy(d, p):
        who, block = zh * 4 + lax.rem(y + d, 4), scaled.at[y, :, pl.ds(*PARTS[p])]
        return rcopy(block, block, ya_send.at[d, p], ya_recv.at[d, p], gz=who)

    def scaled_arrival(d, p):
        who = lax.rem(y + 4 - d, 4)
        block = scaled.at[who, :, pl.ds(*PARTS[p])]
        return rcopy(block, block, ya_send.at[d, p], ya_recv.at[d, p], gz=zh * 4 + who)

    def ssq_copy(d):
        who = zh * 4 + lax.rem(y + d, 4)
        return rcopy(ssq_y.at[0], ssq_y.at[d], sy_send.at[d], sy_recv.at[d], gz=who)

    def ssq_gy_copy(d):
        who = lax.rem(gy + d, 8)
        return rcopy(ssq_gy.at[0], ssq_gy.at[d], sg_send.at[d], sg_recv.at[d], gy=who)

    for p, part in enumerate(PARTS):
        rows = pl.ds(*part)
        zh_copy(p).wait_recv()
        mine = stream[rows] + zh_recv[1, rows].astype(F32)
        theirs = other[rows] + zh_recv[0, rows].astype(F32)
        stream[rows], other[rows] = mine, theirs
        scaled[y, zh, rows] = (mine * gain_ref[...]).astype(BF16)
        scaled[y, 1 - zh, rows] = (theirs * gain_recv[...]).astype(BF16)
        for d in range(1, 4):
            scaled_copy(d, p).start()
    mine, theirs = stream[...], other[...]
    squares = jnp.sum(mine * mine + theirs * theirs, axis=1, keepdims=True)
    squares = jnp.concatenate(
        [jnp.broadcast_to(squares, (ROWS, TILE)), jnp.zeros((256 - ROWS, TILE), F32)], axis=0
    )
    ssq_y[0] = squares.T[:8]
    for d in range(1, 4):
        ssq_copy(d).start()
    last_weights(2)
    pass_weights(4)
    send_own(5)
    for d in range(1, 4):
        for p in range(len(PARTS)):
            scaled_arrival(d, p).wait_recv()
        ssq_copy(d).wait_recv()
    ssq_gy[0] = (ssq_y[0] + ssq_y[1] + ssq_y[2] + ssq_y[3])[:1]
    for d in range(1, 8):
        ssq_gy_copy(d).start()

    weights_here(1)
    weights_here(2)

    def place_of(unit):
        return unit + 2 * lax.min(lax.max(unit - 1, 0), 1) - 5 * lax.min(lax.max(unit - 4, 0), 1)

    def products(unit, parts=(0, 1)):
        columns = pl.ds(pl.multiple_of(place_of(unit) * UNIT, UNIT), UNIT)
        for part in parts:
            w = (wg, wu)[part]
            total = None
            for k in range(4):
                a, b = 2 * k, 2 * k + 1
                left = jnp.concatenate([scaled[a % 4, a // 4], scaled[b % 4, b // 4]], axis=1)
                term = dot(left, w[k * 256 : (k + 1) * 256, columns])
                total = term if total is None else total + term
            for half in range(2):
                gu[unit, 2 * half + part] = total[:, half * TILE : (half + 1) * TILE]

    def r_copy(unit, part):
        return rcopy(
            acc_r.at[unit, part], acc_r.at[unit, part], r_send.at[unit, part], r_recv.at[unit, part],
            gy=up_chip,
        )

    def l_copy(unit, part):
        return rcopy(
            acc_l.at[unit, part], acc_l.at[unit, part], l_send.at[unit, part], l_recv.at[unit, part],
            gy=down_chip,
        )

    def pass_on(tile, unit, copy, acc, first):
        @pl.when(first)
        def _():
            acc[unit, tile] = gu[unit, tile].astype(BF16)

        @pl.when(jnp.logical_not(first))
        def _():
            copy(unit, tile).wait_recv()
            acc[unit, tile] = (gu[unit, tile] + acc[unit, tile].astype(F32)).astype(BF16)

        copy(unit, tile).start()

    def owner_of(unit):
        return unit + lax.min(lax.max(unit - 3, 0), 1)

    def line_step(t, carry):
        right, left = 6 - t + gy, t - 7 + gy

        @pl.when(t == 2)
        def _():
            weights_here(3)
            weights_here(4)

        for tile in range(4):
            if tile == 0:

                @pl.when(t < 4)
                def _():
                    products(lax.select(gy < 4, 6 - t, t))

            @pl.when(jnp.logical_and(t >= gy, owner_of(right) > gy))
            def _():
                pass_on(tile, right, r_copy, acc_r, gy == 0)

            @pl.when(jnp.logical_and(left >= 0, owner_of(left) < gy))
            def _():
                pass_on(tile, left, l_copy, acc_l, gy == 7)

        @pl.when(t < 3)
        def _():
            products(lax.select(gy < 4, t, 6 - t))

        @pl.when(t == 1)
        def _():
            last_weights(3)
            last_weights(4)

        @pl.when(t == 3)
        def _():
            pass_weights(5)

        @pl.when(t == 5)
        def _():
            last_weights(5)

        return carry

    lax.fori_loop(0, 7, line_step, 0)

    for d in range(1, 8):
        ssq_gy_copy(d).wait_recv()
    total = ssq_gy[0]
    for d in range(1, 8):
        total += ssq_gy[d]
    total = lax.rsqrt(total / D + 1e-05)
    inv[...] = jnp.broadcast_to(total, (TILE, 256)).T

    owns = gy != 4
    own_unit = gy - lax.min(lax.max(gy - 4, 0), 1)

    weights_here(5)

    def hidden_copy(unit, k, side, hop):
        half, piece = k // 2, k % 2
        block = hid.at[unit, half, pl.ds(*PIECES[piece])]
        who = lax.max(lax.min(gy + (1 - 2 * side) * hop, 7), 0)
        return rcopy(block, block, h_send.at[unit, side, hop - 1, k], h_recv.at[unit, k], gy=who)

    def hidden_sends(unit, k, side, act):
        room = (7 - gy, gy)[side]
        for hop in (2, 1):

            @pl.when(room >= hop)
            def _():
                act(hidden_copy(unit, k, side, hop))

    def add_down(unit):
        left = jnp.concatenate([hid[unit, 0], hid[unit, 1]], axis=1)
        rows = pl.ds(pl.multiple_of(place_of(unit) * UNIT, UNIT), UNIT)
        for m in range(4):
            down[m] += dot(left, wd[rows, m * 256 : (m + 1) * 256])

    down[...] = jnp.zeros_like(down)

    @pl.when(owns)
    def _():
        for half in range(2):
            for tile in (2 * half, 2 * half + 1):

                @pl.when(gy > 0)
                def _():
                    r_copy(own_unit, tile).wait_recv()
                    gu[own_unit, tile] += acc_r[own_unit, tile].astype(F32)

                @pl.when(gy < 7)
                def _():
                    l_copy(own_unit, tile).wait_recv()
                    gu[own_unit, tile] += acc_l[own_unit, tile].astype(F32)

            gate = inv[:ROWS] * gu[own_unit, 2 * half]
            up = inv[:ROWS] * gu[own_unit, 2 * half + 1]
            hid[own_unit, half] = (gate / (1.0 + jnp.exp(-gate)) * up).astype(BF16)
            for k in (2 * half, 2 * half + 1):
                for side in range(2):
                    hidden_sends(own_unit, k, side, lambda copy: copy.start())

        add_down(own_unit)

    def source(side, far):
        chip = gy - far if side == 0 else gy + far
        there = jnp.logical_and(jnp.logical_and(chip >= 0, chip <= 7), chip != 4)
        return there, chip - lax.min(lax.max(chip - 4, 0), 1)

    def hidden_step(t, carry):
        for k in range(4):
            for side in range(2):
                there, unit = source(side, 2 * t)

                @pl.when(there)
                def _():
                    hidden_copy(unit, k, side, 1).wait_recv()
                    hidden_sends(unit, k, side, lambda copy: copy.start())

        for side in range(2):
            there, unit = source(side, 2 * t - 1)

            @pl.when(there)
            def _():
                for k in range(4):
                    hidden_copy(unit, k, side, 1).wait_recv()
                add_down(unit)

            there, unit = source(side, 2 * t)

            @pl.when(there)
            def _():
                add_down(unit)

        return carry

    lax.fori_loop(1, 5, hidden_step, 0)

    def last_copy(p):
        rows = pl.ds(*PARTS[p])
        return rcopy(zh_send.at[2, rows], zh_recv.at[2, rows], z_send.at[2, p], z_recv.at[2, p], gz=across)

    for p, part in enumerate(PARTS):
        rows = pl.ds(*part)
        for m in range(4):
            keep_tiles(1, m, rows, down[m, rows])
        for d in range(1, 4):
            y_copy(1, d, p).start()
    for p, part in enumerate(PARTS):
        rows = pl.ds(*part)
        for d in range(1, 4):
            y_copy(1, d, p).wait_recv()
        zh_send[2, rows] = y_sum(1, 1 - zh, rows).astype(BF16)
        last_copy(p).start()
        stream[rows] += y_sum(1, zh, rows)
    for d in range(1, 8):
        ssq_gy_copy(d).wait_send()
    for p in range(2):
        attn_far(p).wait_send()
    for d in range(1, 4):
        attn_near(d).wait_send()
        for p in range(2):
            attn_onward(d, p).wait_send()
    for w in range(6):
        for k in range(4):
            w_mate(w, k).wait_send()
    for w in range(6):
        for half in range(2):
            w_copy(w, 0, half).wait_send()
            w_copy(w, 1, half).wait_send()
            w_onward(w, half).wait_send()
    for d in range(1, 4):
        for p in range(len(PARTS)):
            y_copy(0, d, p).wait_send()
            scaled_copy(d, p).wait_send()
        ssq_copy(d).wait_send()
    gain_copy().wait_send()
    for p in range(len(PARTS)):
        zh_copy(p).wait_send()

    def drain(unit, carry):
        owner = owner_of(unit)
        for k in range(4):

            @pl.when(owner > gy)
            def _():
                r_copy(unit, k).wait_send()

            @pl.when(owner < gy)
            def _():
                l_copy(unit, k).wait_send()

            for side, far in ((0, gy - owner), (1, owner - gy)):

                @pl.when(jnp.logical_and(far >= 0, lax.rem(far + 8, 2) == 0))
                def _():
                    hidden_sends(unit, k, side, lambda copy: copy.wait_send())

        return carry

    lax.fori_loop(0, UNITS, drain, 0)

    for p, part in enumerate(PARTS):
        rows = pl.ds(*part)
        last_copy(p).wait_recv()
        out_ref[rows] = (stream[rows] + zh_recv[2, rows].astype(F32)).astype(BF16)
    for p in range(len(PARTS)):
        last_copy(p).wait_send()
        for d in range(1, 4):
            y_copy(1, d, p).wait_send()


def on_device(attn_out, residual, proj_weight, norm_gain, gate_proj, up_proj, down_proj):
    tile = (ROWS, TILE)
    in_vmem, in_hbm = pl.BlockSpec(memory_space=pltpu.VMEM), pl.BlockSpec(memory_space=pl.ANY)
    dma = pltpu.SemaphoreType.DMA
    return pl.pallas_call(
        kernel,
        out_shape=jax.ShapeDtypeStruct(tile, BF16),
        in_specs=[in_hbm] * 7,
        out_specs=in_vmem,
        scratch_shapes=[
            pltpu.VMEM((8, *tile), BF16),
            pltpu.VMEM(tile, BF16),
            pltpu.VMEM((1, TILE), F32),
            pltpu.VMEM((1024, 1024), BF16),
            pltpu.VMEM((1024, 1792), BF16),
            pltpu.VMEM((1024, 1792), BF16),
            pltpu.VMEM((1792, 1024), BF16),
            pltpu.VMEM((8, *tile), F32),
            pltpu.VMEM((2, 4, 2, *tile), BF16),
            pltpu.VMEM((2, 3, 2, *tile), BF16),
            pltpu.VMEM((3, *tile), BF16),
            pltpu.VMEM((3, *tile), BF16),
            pltpu.VMEM((1, TILE), F32),
            pltpu.VMEM(tile, F32),
            pltpu.VMEM(tile, F32),
            pltpu.VMEM((4, 2, *tile), BF16),
            pltpu.VMEM((4, 8, 256), F32),
            pltpu.VMEM((8, 1, 256), F32),
            pltpu.VMEM((256, TILE), F32),
            pltpu.VMEM((UNITS, 4, *tile), F32),
            pltpu.VMEM((UNITS, 4, *tile), BF16),
            pltpu.VMEM((UNITS, 4, *tile), BF16),
            pltpu.VMEM((UNITS, 2, *tile), BF16),
            pltpu.VMEM((4, ROWS, 256), F32),
            dma((9,)), dma((6, 3, 2)), dma((6, 3, 2)), dma((6, 4)), dma((6, 4)),
            dma((4,)), dma((4,)), dma((4, 2)), dma((4, 2)), pltpu.SemaphoreType.REGULAR,
            dma((2, 3, len(PARTS))), dma((2, 3, len(PARTS))), dma((4, len(PARTS))), dma((4, len(PARTS))),
            dma((4,)), dma((4,)), dma((8,)), dma((8,)), dma((3, len(PARTS))), dma((3, len(PARTS))),
            dma((UNITS, 4)), dma((UNITS, 4)), dma((UNITS, 4)), dma((UNITS, 4)),
            dma((UNITS, 2, 2, 4)), dma((UNITS, 4)),
        ],
        compiler_params=pltpu.CompilerParams(
            collective_id=0, has_side_effects=True, vmem_limit_bytes=56 << 20
        ),
    )(attn_out, residual, norm_gain.reshape(1, TILE), proj_weight, gate_proj, up_proj, down_proj)


def solution(mesh):
    in_specs = (
        P("gx", ("gz", "gy")),
        P("gx", ("gy", "gz")),
        P(("gz", "gx"), "gy"),
        P(("gy", "gz")),
        P(("gy", "gx"), "gz"),
        P(("gy", "gx"), "gz"),
        P(("gz", "gx"), "gy"),
    )
    return jax.shard_map(
        on_device, mesh=mesh, in_specs=in_specs, out_specs=P("gx", ("gy", "gz")), check_vma=False
    )
```
